8 devices in a mesh: cp: 8 (over z, y, x, core).
Axes of the slice: x: 2, y: 2, z: 1, core: 2. Of those that a mesh axis runs over, the one named last changes fastest.
Arguments:
- queries: bfloat16 [1024, 128, 192], P('cp')
- latent: bfloat16 [1024, 512], P('cp')
- key_rope: bfloat16 [1024, 64], P('cp')
- w_uk: bfloat16 [512, 128, 128], replicated
- w_uv: bfloat16 [512, 128, 128], replicated
- d_out: bfloat16 [1024, 128, 128], P('cp')
Outputs:
- output 1: bfloat16 [1024, 128, 128], P('cp')
- output 2: bfloat16 [1024, 128, 192], P('cp')
- output 3: bfloat16 [1024, 512], P('cp')
- output 4: bfloat16 [1024, 64], P('cp')
- output 5: float32 [512, 128, 128], replicated
- output 6: float32 [512, 128, 128], replicated
All inputs are finite; a program needn't handle non-finite values.
Results may differ from the reference program's by a relative error of at most 0.014118.
Values are sent between devices in bfloat16 or wider.
A program may use at most 1 GiB of HBM per device.

```python
import math
import jax
import jax.numpy as jnp
from jax import lax

TOK_DEV = 128
N_DEV = 8
N_HEADS = 128
LATENT = 512
NOPE_DIM = 128
ROPE_DIM = 64
V_DIM = 128

SEQ_LEN = TOK_DEV * N_DEV
QK_DIM = NOPE_DIM + ROPE_DIM
SOFT_SCALE = 1.0 / math.sqrt(QK_DIM)
Q_SPREAD = math.sqrt(0.75 * math.log(SEQ_LEN))


def setup_inputs(seed: int = 0) -> dict:
    rng_keys = jax.random.split(jax.random.key(seed), 6)
    queries = jax.random.normal(rng_keys[0], (SEQ_LEN, N_HEADS, QK_DIM), jnp.float32) * Q_SPREAD
    latent = jax.random.normal(rng_keys[1], (SEQ_LEN, LATENT), jnp.float32)
    key_rope = jax.random.normal(rng_keys[2], (SEQ_LEN, ROPE_DIM), jnp.float32)
    w_uk = jax.random.normal(rng_keys[3], (LATENT, N_HEADS, NOPE_DIM), jnp.float32) * LATENT ** -0.5
    w_uv = jax.random.normal(rng_keys[4], (LATENT, N_HEADS, V_DIM), jnp.float32) * LATENT ** -0.5
    d_out = jax.random.normal(rng_keys[5], (SEQ_LEN, N_HEADS, V_DIM), jnp.float32)
    return {
        "queries": queries.astype(jnp.bfloat16),
        "latent": latent.astype(jnp.bfloat16),
        "key_rope": key_rope.astype(jnp.bfloat16),
        "w_uk": w_uk.astype(jnp.bfloat16),
        "w_uv": w_uv.astype(jnp.bfloat16),
        "d_out": d_out.astype(jnp.bfloat16),
    }


def decompress(latent, w_uk, w_uv):
    lat_f = latent.astype(jnp.float32)
    k_nope = jnp.einsum("tl,lhd->thd", lat_f, w_uk.astype(jnp.float32)).astype(jnp.bfloat16)
    values = jnp.einsum("tl,lhd->thd", lat_f, w_uv.astype(jnp.float32)).astype(jnp.bfloat16)
    return k_nope, values


def attend(queries, latent, key_rope, w_uk, w_uv):
    k_nope, values = decompress(latent, w_uk, w_uv)
    k_f = k_nope.astype(jnp.float32)
    v_f = values.astype(jnp.float32)
    r_f = key_rope.astype(jnp.float32)
    key_pos = jnp.arange(SEQ_LEN)

    def block_rows(blk_pair):
        q_blk, q_start = blk_pair
        q_f = q_blk.astype(jnp.float32)
        scores = (jnp.einsum("qhd,khd->hqk", q_f[:, :, :NOPE_DIM], k_f)
                  + jnp.einsum("qhd,kd->hqk", q_f[:, :, NOPE_DIM:], r_f)) * SOFT_SCALE
        q_pos = q_start + jnp.arange(TOK_DEV)
        visible = key_pos[None, :] <= q_pos[:, None]
        scores = jnp.where(visible[None], scores, -1e30)
        attn_prob = jax.nn.softmax(scores, axis=-1)
        return jnp.einsum("hqk,khd->qhd", attn_prob, v_f)

    q_blocks = queries.reshape(N_DEV, TOK_DEV, N_HEADS, QK_DIM)
    q_starts = jnp.arange(N_DEV) * TOK_DEV
    out_rows = lax.map(jax.checkpoint(block_rows), (q_blocks, q_starts))
    return out_rows.reshape(SEQ_LEN, N_HEADS, V_DIM).astype(jnp.bfloat16)


def reference(queries, latent, key_rope, w_uk, w_uv, d_out):
    attn_out, pull_back = jax.vjp(attend, queries, latent, key_rope, w_uk.astype(jnp.float32), w_uv.astype(jnp.float32))
    d_query, d_latent, d_key_rope, d_w_uk, d_w_uv = pull_back(d_out)
    return (attn_out, d_query.astype(jnp.bfloat16), d_latent.astype(jnp.bfloat16), d_key_rope.astype(jnp.bfloat16), d_w_uk, d_w_uv)
```

```python
import functools
import math
import jax
import jax.numpy as jnp
from jax import lax
from jax.experimental import pallas as pl
from jax.experimental.pallas import tpu as pltpu
from jax.sharding import PartitionSpec as P


TB = 128
ND = 8
S = TB * ND
QB = 256
NQ = S // QB
HC = 8
NP = HC // 2
L = 512
D = 128
R = 64
ROWS = 64
NEG = -1e30
BF = jnp.bfloat16
F32 = jnp.float32


def dot(a, b, ca, cb):
    return lax.dot_general(a, b, (((ca,), (cb,)), ((), ())), preferred_element_type=F32)


def pack_kernel(core_ref, qo_ref, do_ref, qp_ref, dp_ref, own_ref, oth_ref, qs, rs, ds):
    for q_ref, g_ref, out in ((qo_ref, do_ref, own_ref), (qp_ref, dp_ref, oth_ref)):
        qs[...] = q_ref[:, :, :D].astype(F32).reshape(TB * HC, D)
        rs[:, :R] = q_ref[:, :, D:].astype(F32).reshape(TB * HC, R)
        ds[...] = g_ref[...].astype(F32).reshape(TB * HC, D)
        for p in range(NP):
            ropes = []
            for k in range(2):
                h = 2 * p + k
                rows = pl.ds(h, TB, stride=HC)
                out[p, k] = qs[rows, :].astype(BF)
                out[p, 2 + k] = ds[rows, :].astype(BF)
                ropes.append(rs[rows, :][:, :R])
            out[p, 4] = jnp.concatenate(ropes, axis=1).astype(BF)


def pack_chunk(j, core, queries, d_out):
    def own(i, c):
        return (0, c[0] * (64 // HC) + j, 0)

    def oth(i, c):
        return (0, (1 - c[0]) * (64 // HC) + j, 0)

    shape = jax.ShapeDtypeStruct((NP, 5, TB, D), BF)
    spec = pl.BlockSpec((NP, 5, TB, D), lambda i, c: (0, 0, 0, 0))
    return pl.pallas_call(
        pack_kernel,
        grid_spec=pltpu.PrefetchScalarGridSpec(
            num_scalar_prefetch=1, grid=(1,),
            in_specs=[pl.BlockSpec((TB, HC, D + R), own), pl.BlockSpec((TB, HC, D), own),
                      pl.BlockSpec((TB, HC, D + R), oth), pl.BlockSpec((TB, HC, D), oth)],
            out_specs=[spec, spec],
            scratch_shapes=[pltpu.VMEM((TB * HC, D), F32)] * 3),
        out_shape=[shape, shape],
        name="pack",
        cost_estimate=pl.CostEstimate(flops=10 ** 9, bytes_accessed=3 * 10 ** 6, transcendentals=0),
    )(core, queries, d_out, queries, d_out)


def prep_kernel(me_ref, *refs):
    ins, (c_ref, ct_ref, r_ref) = refs[:ND], refs[ND:]
    for d in range(ND):
        slot = pl.multiple_of(jnp.bitwise_xor(me_ref[0], d) * TB, TB)
        c = ins[d][:, :L]
        c_ref[pl.ds(slot, TB), :] = c
        ct_ref[:, pl.ds(slot, TB)] = c.astype(F32).T.astype(BF)
        r_ref[pl.ds(slot, TB), :] = ins[d][:, L:]


def prep(me, blocks):
    return pl.pallas_call(
        prep_kernel,
        grid_spec=pltpu.PrefetchScalarGridSpec(
            num_scalar_prefetch=1, grid=(1,),
            in_specs=[pl.BlockSpec((TB, L + D), lambda i, m: (0, 0))] * ND,
            out_specs=[pl.BlockSpec((S, L), lambda i, m: (0, 0)),
                       pl.BlockSpec((L, S), lambda i, m: (0, 0)),
                       pl.BlockSpec((S, D), lambda i, m: (0, 0))]),
        out_shape=[jax.ShapeDtypeStruct((S, L), BF), jax.ShapeDtypeStruct((L, S), BF),
                   jax.ShapeDtypeStruct((S, D), BF)],
        name="prep",
    )(me, *blocks)


def main_kernel(aliased, score_scale, me_ref, *refs):
    n_big = 4 if aliased else 0
    a_refs = refs[:ND]
    c_ref, ct_ref, r_ref, wk_ref, wv_ref, dc_in, dr_in = refs[ND:ND + 7]
    outs = refs[ND + 7 + n_big:]
    (dwk_big, dwv_big, o_big, dq_big, dwk_out, dwv_out, o_par, dq_par, dc_out, dr_out,
     wsc, wk, wv, kr, vs, qa, do, pt, dst, st, dp, dkr, dkb, dvb, osc, dqn, dqr, oacc, dqacc) = outs
    me = me_ref[0]
    core = jnp.bitwise_and(me, 1)
    chip = me // 2
    p = pl.program_id(0)
    own_rows = pl.ds(pl.multiple_of(chip * QB, QB), QB)
    k2 = score_scale * math.log2(math.e)

    @pl.when(p == 0)
    def _():
        for src, dst_w in ((wk_ref, wk), (wv_ref, wv)):
            wsc[...] = src[...].astype(F32).reshape(L * HC, D)
            for h in range(HC):
                dst_w[h // 2, :, (h % 2) * D:(h % 2 + 1) * D] = wsc[pl.ds(h, L, stride=HC), :].astype(BF)
        r = r_ref[...]
        zero = jnp.zeros((S, R), BF)
        kr[0, :, D:] = jnp.concatenate([r[:, :R], zero], axis=1)
        kr[1, :, D:] = jnp.concatenate([zero, r[:, :R]], axis=1)
        pt[...] = jnp.zeros_like(pt)
        dst[...] = jnp.zeros_like(dst)
        dc_out[...] = dc_in[...]
        dr_out[...] = dr_in[...]

    for d in range(ND):
        slot = pl.ds(pl.multiple_of(jnp.bitwise_xor(me, d) * TB, TB), TB)
        for k in range(2):
            qa[k, slot, :D] = a_refs[d][0, k]
            qa[k, slot, D:] = a_refs[d][0, 4]
            do[k, slot, :] = a_refs[d][0, 2 + k]

    for t in range(NQ):
        rows = slice(t * QB, (t + 1) * QB)
        keys = dot(c_ref[rows, :], wk[p], 1, 0).astype(BF)
        vals = dot(c_ref[rows, :], wv[p], 1, 0).astype(BF)
        for k in range(2):
            kr[k, rows, :D] = keys[:, k * D:(k + 1) * D]
            vs[k, rows, :] = vals[:, k * D:(k + 1) * D]

    upper = lax.broadcasted_iota(jnp.int32, (QB, QB), 0) <= lax.broadcasted_iota(jnp.int32, (QB, QB), 1)

    @pl.loop(0, 2)
    def _(k):
        for i in range(NQ):
            n = (i + 1) * QB
            q_i = qa[k, i * QB:n, :]
            d_i = do[k, i * QB:n, :]
            for t in range(i + 1):
                rows = slice(t * QB, (t + 1) * QB)
                sc = dot(kr[k, rows, :], q_i, 1, 1)
                st[rows, :] = jnp.where(upper, sc, NEG) if t == i else sc
                dp[rows, :] = dot(vs[k, rows, :], d_i, 1, 1)
            mx = st[:8, :]
            for r0 in range(8, n, 8):
                mx = jnp.maximum(mx, st[r0:r0 + 8, :])
            mx = jnp.max(mx, axis=0, keepdims=True)
            ls = jnp.zeros((8, QB), F32)
            ts = jnp.zeros((8, QB), F32)
            for r0 in range(0, n, ROWS):
                e = jnp.exp2((st[r0:r0 + ROWS, :] - mx) * k2)
                st[r0:r0 + ROWS, :] = e
                ls += jnp.sum(e.reshape(ROWS // 8, 8, QB), axis=0)
                ts += jnp.sum((e * dp[r0:r0 + ROWS, :]).reshape(ROWS // 8, 8, QB), axis=0)
            inv = 1.0 / jnp.sum(ls, axis=0, keepdims=True)
            delta = jnp.sum(ts, axis=0, keepdims=True) * inv
            for r0 in range(0, n, ROWS):
                prob = st[r0:r0 + ROWS, :] * inv
                pt[r0:r0 + ROWS, i * QB:n] = prob.astype(BF)
                dst[r0:r0 + ROWS, i * QB:n] = (prob * (dp[r0:r0 + ROWS, :] - delta)).astype(BF)

        for t in range(NQ):
            rows = slice(t * QB, (t + 1) * QB)
            grad = dot(dst[rows, t * QB:], qa[k, t * QB:, :], 1, 0) * score_scale
            dkr[rows, :] = grad[:, D:]
            dkb[k, rows, :] = grad[:, :D].astype(BF)
            dvb[k, rows, :] = dot(pt[rows, t * QB:], do[k, t * QB:, :], 1, 0).astype(BF)
        dr_out[k] += dkr[own_rows, :]

        cols = pl.ds(pl.multiple_of(chip * QB, QB), QB)
        oacc[...] = dot(pt[:, cols], vs[k], 0, 0)
        dqacc[...] = dot(dst[:, cols], kr[k], 0, 0) * score_scale
        head = 2 * p + k
        for side in range(2):
            half = jnp.bitwise_xor(core, side)
            tok = pl.ds(pl.multiple_of(half * TB, TB), TB)
            rows = pl.ds(head, TB, stride=HC)
            osc[side, rows, :] = oacc[tok, :]
            dqn[side, rows, :] = dqacc[tok, :D]
            rope = dqacc[tok, D:]
            dqr[side, rows, :] = jnp.where(k == 0, rope, pltpu.roll(rope, R, 1))

    for w, grad_b, big, out in ((wk, dkb, dwk_big, dwk_out), (wv, dvb, dwv_big, dwv_out)):
        own = jnp.concatenate([grad_b[0, own_rows, :], grad_b[1, own_rows, :]], axis=1)
        dc_out[...] += dot(own, w[p], 1, 1)
        both = jnp.concatenate([grad_b[0], grad_b[1]], axis=1)
        for t in range(2):
            rows = slice(t * QB, (t + 1) * QB)
            dw = dot(ct_ref[rows, :], both, 1, 0)
            for k in range(2):
                view = pl.ds(t * QB * HC + 2 * p + k, QB, stride=HC)
                big.reshape(L * HC, D)[view, :] = dw[:, k * D:(k + 1) * D]
                out.reshape(L * HC, D)[view, :] = dw[:, k * D:(k + 1) * D]

    @pl.when(p == NP - 1)
    def _():
        o_big[...] = osc[0].reshape(TB, HC, D).astype(BF)
        o_par[...] = osc[1].reshape(TB, HC, D).astype(BF)
        for side, dq in ((0, dq_big), (1, dq_par)):
            dq[:, :, :D] = dqn[side].reshape(TB, HC, D).astype(BF)
            dq[:, :, D:] = dqr[side].reshape(TB, HC, D)[:, :, :R].astype(BF)


def big_shapes():
    return [jax.ShapeDtypeStruct((L, 128, D), F32), jax.ShapeDtypeStruct((L, 128, D), F32),
            jax.ShapeDtypeStruct((TB, 128, D), BF), jax.ShapeDtypeStruct((TB, 128, D + R), BF)]


def main_chunk(j, score_scale, me, blocks, c_abs, c_t, r_abs, w_uk, w_uv, dc, dr, big):
    def head_block(i, m):
        return (0, (m[0] % 2) * (64 // HC) + j, 0)

    def full2(i, m):
        return (0, 0)

    def full3(i, m):
        return (0, 0, 0)

    aliased = big is not None
    once = pl.Buffered(1)
    in_specs = ([pl.BlockSpec((1, 5, TB, D), lambda i, m: (i, 0, 0, 0))] * ND
                + [pl.BlockSpec((S, L), full2, pipeline_mode=once),
                   pl.BlockSpec((L, S), full2, pipeline_mode=once),
                   pl.BlockSpec((S, D), full2, pipeline_mode=once),
                   pl.BlockSpec((L, HC, D), head_block, pipeline_mode=once),
                   pl.BlockSpec((L, HC, D), head_block, pipeline_mode=once),
                   pl.BlockSpec((QB, L), full2, pipeline_mode=once),
                   pl.BlockSpec((2, QB, D), full3, pipeline_mode=once)])
    args = list(blocks) + [c_abs, c_t, r_abs, w_uk, w_uv, dc, dr]
    aliases = {}
    if aliased:
        in_specs += [pl.BlockSpec(memory_space=pl.ANY)] * 4
        aliases = {1 + len(args) + b: b for b in range(4)}
        args += list(big)
    outs = pl.pallas_call(
        functools.partial(main_kernel, aliased, score_scale),
        grid_spec=pltpu.PrefetchScalarGridSpec(
            num_scalar_prefetch=1, grid=(NP,),
            in_specs=in_specs,
            out_specs=[pl.BlockSpec((L, HC, D), head_block, pipeline_mode=once),
                       pl.BlockSpec((L, HC, D), head_block, pipeline_mode=once),
                       pl.BlockSpec((TB, HC, D), head_block, pipeline_mode=once),
                       pl.BlockSpec((TB, HC, D + R), head_block, pipeline_mode=once),
                       pl.BlockSpec((L, HC, D), full3, pipeline_mode=once),
                       pl.BlockSpec((L, HC, D), full3, pipeline_mode=once),
                       pl.BlockSpec((TB, HC, D), full3, pipeline_mode=once),
                       pl.BlockSpec((TB, HC, D + R), full3, pipeline_mode=once),
                       pl.BlockSpec((QB, L), full2, pipeline_mode=once),
                       pl.BlockSpec((2, QB, D), full3, pipeline_mode=once)],
            scratch_shapes=[
                pltpu.VMEM((L * HC, D), F32),
                pltpu.VMEM((NP, L, 2 * D), BF), pltpu.VMEM((NP, L, 2 * D), BF),
                pltpu.VMEM((2, S, 2 * D), BF), pltpu.VMEM((2, S, D), BF),
                pltpu.VMEM((2, S, 2 * D), BF), pltpu.VMEM((2, S, D), BF),
                pltpu.VMEM((S, S), BF), pltpu.VMEM((S, S), BF),
                pltpu.VMEM((S, QB), F32), pltpu.VMEM((S, QB), F32),
                pltpu.VMEM((S, D), F32),
                pltpu.VMEM((2, S, D), BF), pltpu.VMEM((2, S, D), BF),
                pltpu.VMEM((2, TB * HC, D), F32), pltpu.VMEM((2, TB * HC, D), F32),
                pltpu.VMEM((2, TB * HC, D), F32),
                pltpu.VMEM((QB, D), F32), pltpu.VMEM((QB, 2 * D), F32)]),
        out_shape=big_shapes() + [
            jax.ShapeDtypeStruct((L, HC, D), F32), jax.ShapeDtypeStruct((L, HC, D), F32),
            jax.ShapeDtypeStruct((TB, HC, D), BF), jax.ShapeDtypeStruct((TB, HC, D + R), BF),
            jax.ShapeDtypeStruct((QB, L), F32), jax.ShapeDtypeStruct((2, QB, D), F32)],
        input_output_aliases=aliases,
        compiler_params=pltpu.CompilerParams(vmem_limit_bytes=60 * 2 ** 20),
        name="mla_chunk",
        cost_estimate=pl.CostEstimate(flops=25 * 10 ** 9, bytes_accessed=20 * 10 ** 6, transcendentals=0),
    )(me, *args)
    return outs[:4], outs[4:8], outs[8], outs[9]


def place_kernel(core_ref, *refs):
    ins, outs = refs[:4], refs[8:]
    for a, b in zip(ins, outs):
        b[...] = a[...]


def place(j, core, received, big):
    def at(i, c):
        return (i, (1 - c[0]) * (64 // HC) + j, 0)

    def src(i, c):
        return (i, 0, 0)

    steps = 4
    shapes = [(L // steps, HC, D), (L // steps, HC, D), (TB // steps, HC, D), (TB // steps, HC, D + R)]
    return pl.pallas_call(
        place_kernel,
        grid_spec=pltpu.PrefetchScalarGridSpec(
            num_scalar_prefetch=1, grid=(steps,),
            in_specs=[pl.BlockSpec(s, src) for s in shapes] + [pl.BlockSpec(memory_space=pl.ANY)] * 4,
            out_specs=[pl.BlockSpec(s, at) for s in shapes]),
        out_shape=big_shapes(),
        input_output_aliases={5 + b: b for b in range(4)},
        name="place",
        cost_estimate=pl.CostEstimate(flops=2 * 10 ** 9, bytes_accessed=10 ** 7, transcendentals=0),
    )(core, *received, *big)


def solution(mesh):
    def hop(x, k):
        return lax.ppermute(x, "cp", [(i, i ^ k) for i in range(ND)])

    def local_step(queries, latent, key_rope, w_uk, w_uv, d_out):
        score_scale = 1.0 / math.sqrt(queries.shape[-1])
        dev = lax.axis_index("cp").astype(jnp.int32)
        me = dev[None]
        core = me % 2
        n_chunks = queries.shape[1] // 2 // HC

        lat = jnp.concatenate([latent, key_rope, jnp.zeros((TB, D - R), BF)], axis=1)
        lats = [lat] + [hop(lat, k) for k in range(1, ND)]
        c_abs, c_t, r_abs = prep(me, lats)

        recv = []
        for j in range(n_chunks):
            own, oth = pack_chunk(j, core, queries, d_out)
            if j >= 2:
                own, oth, _, _ = lax.optimization_barrier((own, oth, recv[j - 2][2], recv[j - 2][5]))
            a1, a2, a5, a3, a4 = hop(oth, 1), hop(own, 2), hop(oth, 5), hop(oth, 3), hop(own, 4)
            a6, a7 = hop(a2, 4), hop(a5, 2)
            recv.append([own, a1, a2, a3, a4, a5, a6, a7])

        dc = jnp.zeros((QB, L), F32)
        dr = jnp.zeros((2, QB, D), F32)
        big = None
        pending = None
        for j in range(n_chunks):
            big, send, dc, dr = main_chunk(j, score_scale, me, recv[j], c_abs, c_t, r_abs,
                                           w_uk, w_uv, dc, dr, big)
            if pending is not None:
                big = place(j - 1, core, pending, big)
            pending = [hop(x, 1) for x in send]
        dc = dc.reshape(2, TB, L)
        dr = dr[0, :, :R] + dr[1, :, R:]
        dr = dr.reshape(2, TB, R)
        c_idx = core[0]

        def swap_sum(x):
            mine = lax.dynamic_index_in_dim(x, c_idx, 0, keepdims=False)
            theirs = lax.dynamic_index_in_dim(x, 1 - c_idx, 0, keepdims=False)
            return (mine + hop(theirs, 1)).astype(BF)

        d_latent = swap_sum(dc)
        d_key_rope = swap_sum(dr)
        d_w_uk, d_w_uv, attn_out, d_query = place(n_chunks - 1, core, pending, big)
        return attn_out, d_query, d_latent, d_key_rope, d_w_uk, d_w_uv

    seq = P("cp")
    return jax.shard_map(local_step, mesh=mesh,
                         in_specs=(seq, seq, seq, P(), P(), seq),
                         out_specs=(seq, seq, seq, seq, P(), P()),
                         check_vma=False)
```

```python
import functools
import math
import jax
import jax.numpy as jnp
from jax import lax
from jax.experimental import pallas as pl
from jax.experimental.pallas import tpu as pltpu
from jax.sharding import PartitionSpec as P


TB = 128
ND = 8
S = TB * ND
QB = 256
NQ = S // QB
HC = 8
NP = HC // 2
L = 512
D = 128
R = 64
ROWS = 32
NEG = -1e30
BF = jnp.bfloat16
F32 = jnp.float32


def dot(a, b, ca, cb):
    return lax.dot_general(a, b, (((ca,), (cb,)), ((), ())), preferred_element_type=F32)


def pack_kernel(core_ref, qo_ref, do_ref, qp_ref, dp_ref, own_ref, oth_ref, qs, rs, ds):
    for q_ref, g_ref, out in ((qo_ref, do_ref, own_ref), (qp_ref, dp_ref, oth_ref)):
        qs[...] = q_ref[:, :, :D].astype(F32).reshape(TB * HC, D)
        rs[:, :R] = q_ref[:, :, D:].astype(F32).reshape(TB * HC, R)
        ds[...] = g_ref[...].astype(F32).reshape(TB * HC, D)
        for p in range(NP):
            ropes = []
            for k in range(2):
                h = 2 * p + k
                rows = pl.ds(h, TB, stride=HC)
                out[p, k] = qs[rows, :].astype(BF)
                out[p, 2 + k] = ds[rows, :].astype(BF)
                ropes.append(rs[rows, :][:, :R])
            out[p, 4] = jnp.concatenate(ropes, axis=1).astype(BF)


def pack_chunk(j, core, queries, d_out):
    def own(i, c):
        return (0, c[0] * (64 // HC) + j, 0)

    def oth(i, c):
        return (0, (1 - c[0]) * (64 // HC) + j, 0)

    shape = jax.ShapeDtypeStruct((NP, 5, TB, D), BF)
    spec = pl.BlockSpec((NP, 5, TB, D), lambda i, c: (0, 0, 0, 0))
    return pl.pallas_call(
        pack_kernel,
        grid_spec=pltpu.PrefetchScalarGridSpec(
            num_scalar_prefetch=1, grid=(1,),
            in_specs=[pl.BlockSpec((TB, HC, D + R), own), pl.BlockSpec((TB, HC, D), own),
                      pl.BlockSpec((TB, HC, D + R), oth), pl.BlockSpec((TB, HC, D), oth)],
            out_specs=[spec, spec],
            scratch_shapes=[pltpu.VMEM((TB * HC, D), F32)] * 3),
        out_shape=[shape, shape],
        name="pack",
        cost_estimate=pl.CostEstimate(flops=10 ** 9, bytes_accessed=3 * 10 ** 6, transcendentals=0),
    )(core, queries, d_out, queries, d_out)


def prep_kernel(me_ref, *refs):
    ins, (c_ref, ct_ref, r_ref) = refs[:ND], refs[ND:]
    for d in range(ND):
        slot = pl.multiple_of(jnp.bitwise_xor(me_ref[0], d) * TB, TB)
        c = ins[d][:, :L]
        c_ref[pl.ds(slot, TB), :] = c
        ct_ref[:, pl.ds(slot, TB)] = c.astype(F32).T.astype(BF)
        r_ref[pl.ds(slot, TB), :] = ins[d][:, L:]


def prep(me, blocks):
    return pl.pallas_call(
        prep_kernel,
        grid_spec=pltpu.PrefetchScalarGridSpec(
            num_scalar_prefetch=1, grid=(1,),
            in_specs=[pl.BlockSpec((TB, L + D), lambda i, m: (0, 0))] * ND,
            out_specs=[pl.BlockSpec((S, L), lambda i, m: (0, 0)),
                       pl.BlockSpec((L, S), lambda i, m: (0, 0)),
                       pl.BlockSpec((S, D), lambda i, m: (0, 0))]),
        out_shape=[jax.ShapeDtypeStruct((S, L), BF), jax.ShapeDtypeStruct((L, S), BF),
                   jax.ShapeDtypeStruct((S, D), BF)],
        name="prep",
    )(me, *blocks)


def main_kernel(aliased, score_scale, me_ref, *refs):
    n_big = 4 if aliased else 0
    a_refs = refs[:ND]
    c_ref, ct_ref, r_ref, wk_ref, wv_ref, dc_in, dr_in = refs[ND:ND + 7]
    outs = refs[ND + 7 + n_big:]
    (dwk_big, dwv_big, o_big, dq_big, dwk_out, dwv_out, o_par, dq_par, dc_out, dr_out,
     wsc, wk, wv, kr, vs, qa, do, pt, dst, st, dp, dkr, dkb, dvb, osc, dqn, dqr, oacc, dqacc) = outs
    me = me_ref[0]
    core = jnp.bitwise_and(me, 1)
    chip = me // 2
    p = pl.program_id(0)
    own_rows = pl.ds(pl.multiple_of(chip * QB, QB), QB)
    k2 = score_scale * math.log2(math.e)

    @pl.when(p == 0)
    def _():
        for src, dst_w in ((wk_ref, wk), (wv_ref, wv)):
            wsc[...] = src[...].astype(F32).reshape(L * HC, D)
            for h in range(HC):
                dst_w[h // 2, :, (h % 2) * D:(h % 2 + 1) * D] = wsc[pl.ds(h, L, stride=HC), :].astype(BF)
        r = r_ref[...]
        zero = jnp.zeros((S, R), BF)
        kr[0, :, D:] = jnp.concatenate([r[:, :R], zero], axis=1)
        kr[1, :, D:] = jnp.concatenate([zero, r[:, :R]], axis=1)
        for t in range(1, NQ):
            pt[t * QB:(t + 1) * QB, :t * QB] = jnp.zeros((QB, t * QB), BF)
            dst[t * QB:(t + 1) * QB, :t * QB] = jnp.zeros((QB, t * QB), BF)
        dc_out[...] = dc_in[...]
        dr_out[...] = dr_in[...]

    for d in range(ND):
        slot = pl.ds(pl.multiple_of(jnp.bitwise_xor(me, d) * TB, TB), TB)
        for k in range(2):
            qa[k, slot, :D] = a_refs[d][0, k]
            qa[k, slot, D:] = a_refs[d][0, 4]
            do[k, slot, :] = a_refs[d][0, 2 + k]

    for t in range(NQ):
        rows = slice(t * QB, (t + 1) * QB)
        keys = dot(c_ref[rows, :], wk[p], 1, 0).astype(BF)
        vals = dot(c_ref[rows, :], wv[p], 1, 0).astype(BF)
        for k in range(2):
            kr[k, rows, :D] = keys[:, k * D:(k + 1) * D]
            vs[k, rows, :] = vals[:, k * D:(k + 1) * D]

    upper = lax.broadcasted_iota(jnp.int32, (QB, QB), 0) <= lax.broadcasted_iota(jnp.int32, (QB, QB), 1)

    @pl.loop(0, 2)
    def _(k):
        def scores(i):
            q_i = qa[k, i * QB:(i + 1) * QB, :]
            d_i = do[k, i * QB:(i + 1) * QB, :]
            base = QB * (i * (i + 1) // 2)
            for t in range(i + 1):
                rows = slice(t * QB, (t + 1) * QB)
                out = slice(base + t * QB, base + (t + 1) * QB)
                sc = dot(kr[k, rows, :], q_i, 1, 1)
                st[out, :] = jnp.where(upper, sc, NEG) if t == i else sc
                dp[out, :] = dot(vs[k, rows, :], d_i, 1, 1)

        def soften(i):
            n = (i + 1) * QB
            base = QB * (i * (i + 1) // 2)
            mxs = [st[base + 8 * a:base + 8 * a + 8, :] for a in range(4)]
            for r0 in range(32, n, 32):
                for a in range(4):
                    mxs[a] = jnp.maximum(mxs[a], st[base + r0 + 8 * a:base + r0 + 8 * a + 8, :])
            mx = jnp.maximum(jnp.maximum(mxs[0], mxs[1]), jnp.maximum(mxs[2], mxs[3]))
            mx = jnp.max(mx, axis=0, keepdims=True)
            ls = jnp.zeros((8, QB), F32)
            ts = jnp.zeros((8, QB), F32)
            for r0 in range(base, base + n, ROWS):
                e = jnp.exp2((st[r0:r0 + ROWS, :] - mx) * k2)
                st[r0:r0 + ROWS, :] = e
                ls += jnp.sum(e.reshape(ROWS // 8, 8, QB), axis=0)
                ts += jnp.sum((e * dp[r0:r0 + ROWS, :]).reshape(ROWS // 8, 8, QB), axis=0)
            inv = 1.0 / jnp.sum(ls, axis=0, keepdims=True)
            delta = jnp.sum(ts, axis=0, keepdims=True) * inv
            for r0 in range(0, n, ROWS):
                prob = st[base + r0:base + r0 + ROWS, :] * inv
                pt[r0:r0 + ROWS, i * QB:n] = prob.astype(BF)
                dst[r0:r0 + ROWS, i * QB:n] = (prob * (dp[base + r0:base + r0 + ROWS, :] - delta)).astype(BF)

        def grads(t):
            rows = slice(t * QB, (t + 1) * QB)
            grad = dot(dst[rows, t * QB:], qa[k, t * QB:, :], 1, 0)
            dkr[rows, :] = grad[:, D:]
            dkb[k, rows, :] = grad[:, :D].astype(BF)
            dvb[k, rows, :] = dot(pt[rows, t * QB:], do[k, t * QB:, :], 1, 0).astype(BF)

        scores(NQ - 1)
        for i in range(NQ - 1, -1, -1):
            if i:
                scores(i - 1)
            soften(i)
            grads(i)
        dr_out[k] += dkr[own_rows, :] * score_scale

        cols = pl.ds(pl.multiple_of(chip * QB, QB), QB)
        oacc[...] = dot(pt[:, cols], vs[k], 0, 0)
        dqacc[...] = dot(dst[:, cols], kr[k], 0, 0) * score_scale
        head = 2 * p + k
        for side in range(2):
            half = jnp.bitwise_xor(core, side)
            tok = pl.ds(pl.multiple_of(half * TB, TB), TB)
            rows = pl.ds(head, TB, stride=HC)
            osc[side, rows, :] = oacc[tok, :]
            dqn[side, rows, :] = dqacc[tok, :D]
            rope = dqacc[tok, D:]
            dqr[side, rows, :] = jnp.where(k == 0, rope, pltpu.roll(rope, R, 1))

    for w, grad_b, big, out, mul in ((wk, dkb, dwk_big, dwk_out, score_scale), (wv, dvb, dwv_big, dwv_out, None)):
        own = jnp.concatenate([grad_b[0, own_rows, :], grad_b[1, own_rows, :]], axis=1)
        d_lat = dot(own, w[p], 1, 1)
        dc_out[...] += d_lat if mul is None else d_lat * mul
        both = jnp.concatenate([grad_b[0], grad_b[1]], axis=1)
        for t in range(2):
            rows = slice(t * QB, (t + 1) * QB)
            dw = dot(ct_ref[rows, :], both, 1, 0)
            dw = dw if mul is None else dw * mul
            for k in range(2):
                view = pl.ds(t * QB * HC + 2 * p + k, QB, stride=HC)
                big.reshape(L * HC, D)[view, :] = dw[:, k * D:(k + 1) * D]
                out.reshape(L * HC, D)[view, :] = dw[:, k * D:(k + 1) * D]

    @pl.when(p == NP - 1)
    def _():
        o_big[...] = osc[0].reshape(TB, HC, D).astype(BF)
        o_par[...] = osc[1].reshape(TB, HC, D).astype(BF)
        for side, dq in ((0, dq_big), (1, dq_par)):
            dq[:, :, :D] = dqn[side].reshape(TB, HC, D).astype(BF)
            dq[:, :, D:] = dqr[side].reshape(TB, HC, D)[:, :, :R].astype(BF)


def big_shapes():
    return [jax.ShapeDtypeStruct((L, 128, D), F32), jax.ShapeDtypeStruct((L, 128, D), F32),
            jax.ShapeDtypeStruct((TB, 128, D), BF), jax.ShapeDtypeStruct((TB, 128, D + R), BF)]


def main_chunk(j, score_scale, me, blocks, c_abs, c_t, r_abs, w_uk, w_uv, dc, dr, big):
    def head_block(i, m):
        return (0, (m[0] % 2) * (64 // HC) + j, 0)

    def full2(i, m):
        return (0, 0)

    def full3(i, m):
        return (0, 0, 0)

    aliased = big is not None
    once = pl.Buffered(1)
    in_specs = ([pl.BlockSpec((1, 5, TB, D), lambda i, m: (i, 0, 0, 0))] * ND
                + [pl.BlockSpec((S, L), full2, pipeline_mode=once),
                   pl.BlockSpec((L, S), full2, pipeline_mode=once),
                   pl.BlockSpec((S, D), full2, pipeline_mode=once),
                   pl.BlockSpec((L, HC, D), head_block, pipeline_mode=once),
                   pl.BlockSpec((L, HC, D), head_block, pipeline_mode=once),
                   pl.BlockSpec((QB, L), full2, pipeline_mode=once),
                   pl.BlockSpec((2, QB, D), full3, pipeline_mode=once)])
    args = list(blocks) + [c_abs, c_t, r_abs, w_uk, w_uv, dc, dr]
    aliases = {}
    if aliased:
        in_specs += [pl.BlockSpec(memory_space=pl.ANY)] * 4
        aliases = {1 + len(args) + b: b for b in range(4)}
        args += list(big)
    outs = pl.pallas_call(
        functools.partial(main_kernel, aliased, score_scale),
        grid_spec=pltpu.PrefetchScalarGridSpec(
            num_scalar_prefetch=1, grid=(NP,),
            in_specs=in_specs,
            out_specs=[pl.BlockSpec((L, HC, D), head_block, pipeline_mode=once),
                       pl.BlockSpec((L, HC, D), head_block, pipeline_mode=once),
                       pl.BlockSpec((TB, HC, D), head_block, pipeline_mode=once),
                       pl.BlockSpec((TB, HC, D + R), head_block, pipeline_mode=once),
                       pl.BlockSpec((L, HC, D), full3, pipeline_mode=once),
                       pl.BlockSpec((L, HC, D), full3, pipeline_mode=once),
                       pl.BlockSpec((TB, HC, D), full3, pipeline_mode=once),
                       pl.BlockSpec((TB, HC, D + R), full3, pipeline_mode=once),
                       pl.BlockSpec((QB, L), full2, pipeline_mode=once),
                       pl.BlockSpec((2, QB, D), full3, pipeline_mode=once)],
            scratch_shapes=[
                pltpu.VMEM((L * HC, D), F32),
                pltpu.VMEM((NP, L, 2 * D), BF), pltpu.VMEM((NP, L, 2 * D), BF),
                pltpu.VMEM((2, S, 2 * D), BF), pltpu.VMEM((2, S, D), BF),
                pltpu.VMEM((2, S, 2 * D), BF), pltpu.VMEM((2, S, D), BF),
                pltpu.VMEM((S, S), BF), pltpu.VMEM((S, S), BF),
                pltpu.VMEM((QB * NQ * (NQ + 1) // 2, QB), F32), pltpu.VMEM((QB * NQ * (NQ + 1) // 2, QB), F32),
                pltpu.VMEM((S, D), F32),
                pltpu.VMEM((2, S, D), BF), pltpu.VMEM((2, S, D), BF),
                pltpu.VMEM((2, TB * HC, D), F32), pltpu.VMEM((2, TB * HC, D), F32),
                pltpu.VMEM((2, TB * HC, D), F32),
                pltpu.VMEM((QB, D), F32), pltpu.VMEM((QB, 2 * D), F32)]),
        out_shape=big_shapes() + [
            jax.ShapeDtypeStruct((L, HC, D), F32), jax.ShapeDtypeStruct((L, HC, D), F32),
            jax.ShapeDtypeStruct((TB, HC, D), BF), jax.ShapeDtypeStruct((TB, HC, D + R), BF),
            jax.ShapeDtypeStruct((QB, L), F32), jax.ShapeDtypeStruct((2, QB, D), F32)],
        input_output_aliases=aliases,
        compiler_params=pltpu.CompilerParams(vmem_limit_bytes=60 * 2 ** 20),
        name="mla_chunk",
        cost_estimate=pl.CostEstimate(flops=25 * 10 ** 9, bytes_accessed=20 * 10 ** 6, transcendentals=0),
    )(me, *args)
    return outs[:4], outs[4:8], outs[8], outs[9]


def place_kernel(core_ref, *refs):
    ins, outs = refs[:4], refs[8:]
    for a, b in zip(ins, outs):
        b[...] = a[...]


def place(j, core, received, big):
    def at(i, c):
        return (i, (1 - c[0]) * (64 // HC) + j, 0)

    def src(i, c):
        return (i, 0, 0)

    steps = 4
    shapes = [(L // steps, HC, D), (L // steps, HC, D), (TB // steps, HC, D), (TB // steps, HC, D + R)]
    return pl.pallas_call(
        place_kernel,
        grid_spec=pltpu.PrefetchScalarGridSpec(
            num_scalar_prefetch=1, grid=(steps,),
            in_specs=[pl.BlockSpec(s, src) for s in shapes] + [pl.BlockSpec(memory_space=pl.ANY)] * 4,
            out_specs=[pl.BlockSpec(s, at) for s in shapes]),
        out_shape=big_shapes(),
        input_output_aliases={5 + b: b for b in range(4)},
        name="place",
        cost_estimate=pl.CostEstimate(flops=2 * 10 ** 9, bytes_accessed=10 ** 7, transcendentals=0),
    )(core, *received, *big)


def solution(mesh):
    def hop(x, k):
        perm = [(i, i ^ k) for i in range(ND)]
        return lax.ppermute(x, "cp", perm)

    def step(queries, latent, key_rope, w_uk, w_uv, d_out):
        score_scale = 1.0 / math.sqrt(queries.shape[-1])
        dev = lax.axis_index("cp").astype(jnp.int32)
        me = dev[None]
        core = me % 2
        n_chunks = queries.shape[1] // 2 // HC

        lat = jnp.concatenate([latent, key_rope, jnp.zeros((TB, D - R), BF)], axis=1)
        lats = [lat] + [hop(lat, k) for k in range(1, ND)]
        queries, lat1 = lax.optimization_barrier((queries, lats[1]))
        lats[1] = lat1
        c_abs, c_t, r_abs = prep(me, lats)

        recv = []
        for j in range(n_chunks):
            own, oth = pack_chunk(j, core, queries, d_out)
            a1, a2, a5, a3, a4 = [hop(x, k)
                                  for x, k in ((oth, 1), (own, 2), (oth, 5), (oth, 3), (own, 4))]
            a6, a7 = hop(a2, 4), hop(a5, 2)
            recv.append([own, a1, a2, a3, a4, a5, a6, a7])

        dc = jnp.zeros((QB, L), F32)
        dr = jnp.zeros((2, QB, D), F32)
        big = None
        pending = None
        for j in range(n_chunks):
            big, send, dc, dr = main_chunk(j, score_scale, me, recv[j], c_abs, c_t, r_abs,
                                           w_uk, w_uv, dc, dr, big)
            if pending is not None:
                big = place(j - 1, core, pending, big)
            pending = [hop(x, 1) for x in send]
        dc = dc.reshape(2, TB, L)
        dr = dr[0, :, :R] + dr[1, :, R:]
        dr = dr.reshape(2, TB, R)
        c_idx = core[0]

        def swap_sum(x):
            mine = lax.dynamic_index_in_dim(x, c_idx, 0, keepdims=False)
            theirs = lax.dynamic_index_in_dim(x, 1 - c_idx, 0, keepdims=False)
            return (mine + hop(theirs, 1)).astype(BF)

        d_latent = swap_sum(dc)
        d_key_rope = swap_sum(dr)
        d_w_uk, d_w_uv, attn_out, d_query = place(n_chunks - 1, core, pending, big)
        return attn_out, d_query, d_latent, d_key_rope, d_w_uk, d_w_uv

    seq = P("cp")
    return jax.shard_map(step, mesh=mesh,
                         in_specs=(seq, seq, seq, P(), P(), seq),
                         out_specs=(seq, seq, seq, seq, P(), P()),
                         check_vma=False)
```

```python
import functools
import math
import jax
import jax.numpy as jnp
from jax import lax
from jax.experimental import pallas as pl
from jax.experimental.pallas import tpu as pltpu
from jax.sharding import PartitionSpec as P


TB = 128
ND = 8
S = TB * ND
QB = 256
NQ = S // QB
HC = 8
NP = HC // 2
L = 512
D = 128
R = 64
ROWS = 32
NEG = -1e30
BF = jnp.bfloat16
F32 = jnp.float32


def dot(a, b, ca, cb):
    return lax.dot_general(a, b, (((ca,), (cb,)), ((), ())), preferred_element_type=F32)


def pack_kernel(core_ref, qo_ref, do_ref, qp_ref, dp_ref, own_ref, oth_ref, qs, rs, ds):
    for q_ref, g_ref, out in ((qo_ref, do_ref, own_ref), (qp_ref, dp_ref, oth_ref)):
        qs[...] = q_ref[:, :, :D].astype(F32).reshape(TB * HC, D)
        rs[:, :R] = q_ref[:, :, D:].astype(F32).reshape(TB * HC, R)
        ds[...] = g_ref[...].astype(F32).reshape(TB * HC, D)
        for p in range(NP):
            ropes = []
            for k in range(2):
                h = 2 * p + k
                rows = pl.ds(h, TB, stride=HC)
                out[p, k] = qs[rows, :].astype(BF)
                out[p, 2 + k] = ds[rows, :].astype(BF)
                ropes.append(rs[rows, :][:, :R])
            out[p, 4] = jnp.concatenate(ropes, axis=1).astype(BF)


def pack_chunk(j, core, queries, d_out):
    def own(i, c):
        return (0, c[0] * (64 // HC) + j, 0)

    def oth(i, c):
        return (0, (1 - c[0]) * (64 // HC) + j, 0)

    shape = jax.ShapeDtypeStruct((NP, 5, TB, D), BF)
    spec = pl.BlockSpec((NP, 5, TB, D), lambda i, c: (0, 0, 0, 0))
    return pl.pallas_call(
        pack_kernel,
        grid_spec=pltpu.PrefetchScalarGridSpec(
            num_scalar_prefetch=1, grid=(1,),
            in_specs=[pl.BlockSpec((TB, HC, D + R), own), pl.BlockSpec((TB, HC, D), own),
                      pl.BlockSpec((TB, HC, D + R), oth), pl.BlockSpec((TB, HC, D), oth)],
            out_specs=[spec, spec],
            scratch_shapes=[pltpu.VMEM((TB * HC, D), F32)] * 3),
        out_shape=[shape, shape],
        name="pack",
        cost_estimate=pl.CostEstimate(flops=10 ** 9, bytes_accessed=3 * 10 ** 6, transcendentals=0),
    )(core, queries, d_out, queries, d_out)


def prep_kernel(me_ref, *refs):
    ins, (c_ref, ct_ref, r_ref) = refs[:ND], refs[ND:]
    for d in range(ND):
        slot = pl.multiple_of(jnp.bitwise_xor(me_ref[0], d) * TB, TB)
        c = ins[d][:, :L]
        c_ref[pl.ds(slot, TB), :] = c
        ct_ref[:, pl.ds(slot, TB)] = c.astype(F32).T.astype(BF)
        r_ref[pl.ds(slot, TB), :] = ins[d][:, L:]


def prep(me, blocks):
    return pl.pallas_call(
        prep_kernel,
        grid_spec=pltpu.PrefetchScalarGridSpec(
            num_scalar_prefetch=1, grid=(1,),
            in_specs=[pl.BlockSpec((TB, L + D), lambda i, m: (0, 0))] * ND,
            out_specs=[pl.BlockSpec((S, L), lambda i, m: (0, 0)),
                       pl.BlockSpec((L, S), lambda i, m: (0, 0)),
                       pl.BlockSpec((S, D), lambda i, m: (0, 0))]),
        out_shape=[jax.ShapeDtypeStruct((S, L), BF), jax.ShapeDtypeStruct((L, S), BF),
                   jax.ShapeDtypeStruct((S, D), BF)],
        name="prep",
    )(me, *blocks)


def partner_dw(h0, scale, ct_ref, dkv_in, bigs):
    for w in range(2):
        view = bigs[w].reshape(L * HC, D)
        for t in range(2):
            dw = dot(ct_ref[t * QB:(t + 1) * QB, :], dkv_in[0, w], 1, 0)
            dw = dw * scale if w == 0 else dw
            for k in range(2):
                view[pl.ds(t * QB * HC + h0 + k, QB, stride=HC), :] = dw[:, k * D:(k + 1) * D]


def main_kernel(aliased, prev, score_scale, me_ref, *refs):
    _, ct_ref, _, _, _, _, _ = refs[ND:ND + 7]
    n_in = ND + 7
    if prev:
        dkv_in, o_in, dq_in = refs[n_in:n_in + 3]
        n_in += 3
    outs = refs[n_in + (4 if aliased else 0):]
    (dwk_big, dwv_big, o_big, dq_big, dkv_out, o_par, dq_par, dc_out, dr_out, *scratch) = outs
    step = pl.program_id(0)
    if not prev:
        main_body(step, score_scale, me_ref, refs, outs)
        return

    @pl.when(step < NP)
    def _():
        partner_dw(2 * step, score_scale, ct_ref, dkv_in, (dwk_big, dwv_big))

    @pl.when(step == 0)
    def _():
        o_big[...] = o_in[...]
        dq_big[...] = dq_in[...]

    @pl.when(step >= NP)
    def _():
        main_body(step - NP, score_scale, me_ref, refs, outs)


def main_body(p, score_scale, me_ref, refs, outs):
    a_refs = refs[:ND]
    c_ref, ct_ref, r_ref, wk_ref, wv_ref, dc_in, dr_in = refs[ND:ND + 7]
    (dwk_big, dwv_big, o_big, dq_big, dkv_out, o_par, dq_par, dc_out, dr_out,
     wsc, wk, wv, kr, vs, qa, do, pt, dst, st, dp, dkr, osc, dqn, dqr, oacc, dqacc) = outs
    me = me_ref[0]
    core = jnp.bitwise_and(me, 1)
    chip = me // 2
    own_rows = pl.ds(pl.multiple_of(chip * QB, QB), QB)
    k2 = score_scale * math.log2(math.e)

    @pl.when(p == 0)
    def _():
        for src, dst_w in ((wk_ref, wk), (wv_ref, wv)):
            wsc[...] = src[...].astype(F32).reshape(L * HC, D)
            for h in range(HC):
                dst_w[h // 2, :, (h % 2) * D:(h % 2 + 1) * D] = wsc[pl.ds(h, L, stride=HC), :].astype(BF)
        r = r_ref[...]
        zero = jnp.zeros((S, R), BF)
        kr[0, :, D:] = jnp.concatenate([r[:, :R], zero], axis=1)
        kr[1, :, D:] = jnp.concatenate([zero, r[:, :R]], axis=1)
        for t in range(1, NQ):
            pt[t * QB:(t + 1) * QB, :t * QB] = jnp.zeros((QB, t * QB), BF)
            dst[t * QB:(t + 1) * QB, :t * QB] = jnp.zeros((QB, t * QB), BF)
        dc_out[...] = dc_in[...]
        dr_out[...] = dr_in[...]

    for d in range(ND):
        slot = pl.ds(pl.multiple_of(jnp.bitwise_xor(me, d) * TB, TB), TB)
        for k in range(2):
            qa[k, slot, :D] = a_refs[d][0, k]
            qa[k, slot, D:] = a_refs[d][0, 4]
            do[k, slot, :] = a_refs[d][0, 2 + k]

    for t in range(NQ):
        rows = slice(t * QB, (t + 1) * QB)
        keys = dot(c_ref[rows, :], wk[p], 1, 0).astype(BF)
        vals = dot(c_ref[rows, :], wv[p], 1, 0).astype(BF)
        for k in range(2):
            kr[k, rows, :D] = keys[:, k * D:(k + 1) * D]
            vs[k, rows, :] = vals[:, k * D:(k + 1) * D]

    upper = lax.broadcasted_iota(jnp.int32, (QB, QB), 0) <= lax.broadcasted_iota(jnp.int32, (QB, QB), 1)

    @pl.loop(0, 2)
    def _(k):
        def scores(i):
            q_i = qa[k, i * QB:(i + 1) * QB, :]
            d_i = do[k, i * QB:(i + 1) * QB, :]
            base = QB * (i * (i + 1) // 2)
            for t in range(i + 1):
                rows = slice(t * QB, (t + 1) * QB)
                out = slice(base + t * QB, base + (t + 1) * QB)
                sc = dot(kr[k, rows, :], q_i, 1, 1)
                st[out, :] = jnp.where(upper, sc, NEG) if t == i else sc
                dp[out, :] = dot(vs[k, rows, :], d_i, 1, 1)

        def soften(i):
            n = (i + 1) * QB
            base = QB * (i * (i + 1) // 2)
            mxs = [st[base + 8 * a:base + 8 * a + 8, :] for a in range(4)]
            for r0 in range(32, n, 32):
                for a in range(4):
                    mxs[a] = jnp.maximum(mxs[a], st[base + r0 + 8 * a:base + r0 + 8 * a + 8, :])
            mx = jnp.maximum(jnp.maximum(mxs[0], mxs[1]), jnp.maximum(mxs[2], mxs[3]))
            mx = jnp.max(mx, axis=0, keepdims=True)
            ls = jnp.zeros((8, QB), F32)
            ts = jnp.zeros((8, QB), F32)
            for r0 in range(base, base + n, ROWS):
                e = jnp.exp2((st[r0:r0 + ROWS, :] - mx) * k2)
                st[r0:r0 + ROWS, :] = e
                ls += jnp.sum(e.reshape(ROWS // 8, 8, QB), axis=0)
                ts += jnp.sum((e * dp[r0:r0 + ROWS, :]).reshape(ROWS // 8, 8, QB), axis=0)
            inv = 1.0 / jnp.sum(ls, axis=0, keepdims=True)
            delta = jnp.sum(ts, axis=0, keepdims=True) * inv
            for r0 in range(0, n, ROWS):
                prob = st[base + r0:base + r0 + ROWS, :] * inv
                pt[r0:r0 + ROWS, i * QB:n] = prob.astype(BF)
                dst[r0:r0 + ROWS, i * QB:n] = (prob * (dp[base + r0:base + r0 + ROWS, :] - delta)).astype(BF)

        def grads(t):
            rows = slice(t * QB, (t + 1) * QB)
            grad = dot(dst[rows, t * QB:], qa[k, t * QB:, :], 1, 0)
            dkr[rows, :] = grad[:, D:]
            lanes = pl.ds(pl.multiple_of(k * D, D), D)
            dkv_out[0, 0, rows, lanes] = grad[:, :D].astype(BF)
            dkv_out[0, 1, rows, lanes] = dot(pt[rows, t * QB:], do[k, t * QB:, :], 1, 0).astype(BF)

        scores(NQ - 1)
        for i in range(NQ - 1, -1, -1):
            if i:
                scores(i - 1)
            soften(i)
            grads(i)
        dr_out[k] += dkr[own_rows, :] * score_scale

        cols = pl.ds(pl.multiple_of(chip * QB, QB), QB)
        oacc[...] = dot(pt[:, cols], vs[k], 0, 0)
        dqacc[...] = dot(dst[:, cols], kr[k], 0, 0) * score_scale
        head = 2 * p + k
        for side in range(2):
            half = jnp.bitwise_xor(core, side)
            tok = pl.ds(pl.multiple_of(half * TB, TB), TB)
            rows = pl.ds(head, TB, stride=HC)
            osc[side, rows, :] = oacc[tok, :]
            dqn[side, rows, :] = dqacc[tok, :D]
            rope = dqacc[tok, D:]
            dqr[side, rows, :] = jnp.where(k == 0, rope, pltpu.roll(rope, R, 1))

    for g, w in enumerate((wk, wv)):
        d_lat = dot(dkv_out[0, g, own_rows, :], w[p], 1, 1)
        dc_out[...] += d_lat if g else d_lat * score_scale
    partner_dw(2 * p, score_scale, ct_ref, dkv_out, (dwk_big, dwv_big))

    @pl.when(p == NP - 1)
    def _():
        o_big[...] = osc[0].reshape(TB, HC, D).astype(BF)
        o_par[...] = osc[1].reshape(TB, HC, D).astype(BF)
        for side, dq in ((0, dq_big), (1, dq_par)):
            dq[:, :, :D] = dqn[side].reshape(TB, HC, D).astype(BF)
            dq[:, :, D:] = dqr[side].reshape(TB, HC, D)[:, :, :R].astype(BF)


def big_shapes():
    return [jax.ShapeDtypeStruct((L, 128, D), F32), jax.ShapeDtypeStruct((L, 128, D), F32),
            jax.ShapeDtypeStruct((TB, 128, D), BF), jax.ShapeDtypeStruct((TB, 128, D + R), BF)]


def main_chunk(j, score_scale, me, blocks, c_abs, c_t, r_abs, w_uk, w_uv, dc, dr, big, prev):
    per = 64 // HC
    lead = NP if prev is not None else 0

    def head_block(i, m):
        return (0, (m[0] % 2) * per + j, 0)

    def out_block(i, m):
        own = (m[0] % 2) * per + j
        if not lead:
            return (0, own, 0)
        return (0, jnp.where(i < lead, (1 - m[0] % 2) * per + j - 2, own), 0)

    def main_step(i, m):
        return (jnp.maximum(i - lead, 0), 0, 0, 0)

    def prev_step(i, m):
        return (jnp.minimum(i, NP - 1), 0, 0, 0)

    def full2(i, m):
        return (0, 0)

    def full3(i, m):
        return (0, 0, 0)

    once = pl.Buffered(1)
    in_specs = ([pl.BlockSpec((1, 5, TB, D), main_step)] * ND
                + [pl.BlockSpec((S, L), full2, pipeline_mode=once),
                   pl.BlockSpec((L, S), full2, pipeline_mode=once),
                   pl.BlockSpec((S, D), full2, pipeline_mode=once),
                   pl.BlockSpec((L, HC, D), head_block, pipeline_mode=once),
                   pl.BlockSpec((L, HC, D), head_block, pipeline_mode=once),
                   pl.BlockSpec((QB, L), full2, pipeline_mode=once),
                   pl.BlockSpec((2, QB, D), full3, pipeline_mode=once)])
    args = list(blocks) + [c_abs, c_t, r_abs, w_uk, w_uv, dc, dr]
    if prev is not None:
        in_specs += [pl.BlockSpec((1, 2, S, 2 * D), prev_step),
                     pl.BlockSpec((TB, HC, D), full3, pipeline_mode=once),
                     pl.BlockSpec((TB, HC, D + R), full3, pipeline_mode=once)]
        args += list(prev)
    aliases = {}
    if big is not None:
        in_specs += [pl.BlockSpec(memory_space=pl.ANY)] * 4
        aliases = {1 + len(args) + b: b for b in range(4)}
        args += list(big)
    tri = QB * NQ * (NQ + 1) // 2
    outs = pl.pallas_call(
        functools.partial(main_kernel, big is not None, prev is not None, score_scale),
        grid_spec=pltpu.PrefetchScalarGridSpec(
            num_scalar_prefetch=1, grid=(NP + lead,),
            in_specs=in_specs,
            out_specs=[pl.BlockSpec((L, HC, D), out_block),
                       pl.BlockSpec((L, HC, D), out_block),
                       pl.BlockSpec((TB, HC, D), out_block),
                       pl.BlockSpec((TB, HC, D + R), out_block),
                       pl.BlockSpec((1, 2, S, 2 * D), main_step),
                       pl.BlockSpec((TB, HC, D), full3, pipeline_mode=once),
                       pl.BlockSpec((TB, HC, D + R), full3, pipeline_mode=once),
                       pl.BlockSpec((QB, L), full2, pipeline_mode=once),
                       pl.BlockSpec((2, QB, D), full3, pipeline_mode=once)],
            scratch_shapes=[
                pltpu.VMEM((L * HC, D), F32),
                pltpu.VMEM((NP, L, 2 * D), BF), pltpu.VMEM((NP, L, 2 * D), BF),
                pltpu.VMEM((2, S, 2 * D), BF), pltpu.VMEM((2, S, D), BF),
                pltpu.VMEM((2, S, 2 * D), BF), pltpu.VMEM((2, S, D), BF),
                pltpu.VMEM((S, S), BF), pltpu.VMEM((S, S), BF),
                pltpu.VMEM((tri, QB), F32), pltpu.VMEM((tri, QB), F32),
                pltpu.VMEM((S, D), F32),
                pltpu.VMEM((2, TB * HC, D), F32), pltpu.VMEM((2, TB * HC, D), F32),
                pltpu.VMEM((2, TB * HC, D), F32),
                pltpu.VMEM((QB, D), F32), pltpu.VMEM((QB, 2 * D), F32)]),
        out_shape=big_shapes() + [
            jax.ShapeDtypeStruct((NP, 2, S, 2 * D), BF),
            jax.ShapeDtypeStruct((TB, HC, D), BF), jax.ShapeDtypeStruct((TB, HC, D + R), BF),
            jax.ShapeDtypeStruct((QB, L), F32), jax.ShapeDtypeStruct((2, QB, D), F32)],
        input_output_aliases=aliases,
        compiler_params=pltpu.CompilerParams(vmem_limit_bytes=60 * 2 ** 20),
        name="mla_chunk",
        cost_estimate=pl.CostEstimate(flops=25 * 10 ** 9, bytes_accessed=20 * 10 ** 6, transcendentals=0),
    )(me, *args)
    return outs[:4], outs[4:7], outs[7], outs[8]


def last_kernel(score_scale, core_ref, ct_ref, dkv_in, o_in, dq_in, *refs):
    dwk_big, dwv_big, o_big, dq_big = refs[4:]
    step = pl.program_id(0)
    partner_dw(2 * step, score_scale, ct_ref, dkv_in, (dwk_big, dwv_big))

    @pl.when(step == 0)
    def _():
        o_big[...] = o_in[...]
        dq_big[...] = dq_in[...]


def last_chunk(j, score_scale, core, c_t, prev, big):
    def at(i, c):
        return (0, (1 - c[0]) * (64 // HC) + j, 0)

    def full3(i, c):
        return (0, 0, 0)

    return pl.pallas_call(
        functools.partial(last_kernel, score_scale),
        grid_spec=pltpu.PrefetchScalarGridSpec(
            num_scalar_prefetch=1, grid=(NP,),
            in_specs=[pl.BlockSpec((L, S), lambda i, c: (0, 0), pipeline_mode=pl.Buffered(1)),
                      pl.BlockSpec((1, 2, S, 2 * D), lambda i, c: (i, 0, 0, 0)),
                      pl.BlockSpec((TB, HC, D), full3), pl.BlockSpec((TB, HC, D + R), full3)]
                     + [pl.BlockSpec(memory_space=pl.ANY)] * 4,
            out_specs=[pl.BlockSpec((L, HC, D), at), pl.BlockSpec((L, HC, D), at),
                       pl.BlockSpec((TB, HC, D), at), pl.BlockSpec((TB, HC, D + R), at)]),
        out_shape=big_shapes(),
        input_output_aliases={5 + b: b for b in range(4)},
        compiler_params=pltpu.CompilerParams(vmem_limit_bytes=40 * 2 ** 20),
        name="last",
        cost_estimate=pl.CostEstimate(flops=2 * 10 ** 9, bytes_accessed=10 ** 7, transcendentals=0),
    )(core, c_t, *prev, *big)


def solution(mesh):
    def hop(x, k):
        perm = [(i, i ^ k) for i in range(ND)]
        return lax.ppermute(x, "cp", perm)

    def step(queries, latent, key_rope, w_uk, w_uv, d_out):
        score_scale = 1.0 / math.sqrt(queries.shape[-1])
        dev = lax.axis_index("cp").astype(jnp.int32)
        me = dev[None]
        core = me % 2
        n_chunks = queries.shape[1] // 2 // HC

        lat = jnp.concatenate([latent, key_rope, jnp.zeros((TB, D - R), BF)], axis=1)
        lats = [lat] + [hop(lat, k) for k in range(1, ND)]
        queries, lat1 = lax.optimization_barrier((queries, lats[1]))
        lats[1] = lat1
        c_abs, c_t, r_abs = prep(me, lats)

        packs = [pack_chunk(j, core, queries, d_out) for j in range(n_chunks)]
        me0 = lax.optimization_barrier((me, *[own for own, _ in packs]))[0]
        recv = []
        for own, oth in packs:
            a1, a2, a5, a3, a4 = [hop(x, k)
                                  for x, k in ((oth, 1), (own, 2), (oth, 5), (oth, 3), (own, 4))]
            a6, a7 = hop(a2, 4), hop(a5, 2)
            recv.append([own, a1, a2, a3, a4, a5, a6, a7])

        dc = jnp.zeros((QB, L), F32)
        dr = jnp.zeros((2, QB, D), F32)
        big = None
        sent = []
        for j in range(n_chunks):
            big, send, dc, dr = main_chunk(j, score_scale, me0 if j == 0 else me, recv[j],
                                           c_abs, c_t, r_abs, w_uk, w_uv, dc, dr, big,
                                           sent[j - 2] if j >= 2 else None)
            sent.append([hop(x, 1) for x in send])
        dc = dc.reshape(2, TB, L)
        dr = dr[0, :, :R] + dr[1, :, R:]
        dr = dr.reshape(2, TB, R)
        c_idx = core[0]

        def swap_sum(x):
            mine = lax.dynamic_index_in_dim(x, c_idx, 0, keepdims=False)
            theirs = lax.dynamic_index_in_dim(x, 1 - c_idx, 0, keepdims=False)
            return (mine + hop(theirs, 1)).astype(BF)

        d_latent = swap_sum(dc)
        d_key_rope = swap_sum(dr)
        for j in (n_chunks - 2, n_chunks - 1):
            big = last_chunk(j, score_scale, core, c_t, sent[j], big)
        d_w_uk, d_w_uv, attn_out, d_query = big
        return attn_out, d_query, d_latent, d_key_rope, d_w_uk, d_w_uv

    seq = P("cp")
    return jax.shard_map(step, mesh=mesh,
                         in_specs=(seq, seq, seq, P(), P(), seq),
                         out_specs=(seq, seq, seq, seq, P(), P()),
                         check_vma=False)
```

```python
import functools
import math
import jax
import jax.numpy as jnp
from jax import lax
from jax.experimental import pallas as pl
from jax.experimental.pallas import tpu as pltpu
from jax.sharding import PartitionSpec as P


TB = 128
ND = 8
S = TB * ND
QB = 256
NQ = S // QB
HC = 8
NP = HC // 2
L = 512
D = 128
R = 64
ROWS = 32
NEG = -1e30
BF = jnp.bfloat16
GROUPS = (1, 1, 2, 2, 1, 1)
F32 = jnp.float32


def dot(a, b, ca, cb):
    return lax.dot_general(a, b, (((ca,), (cb,)), ((), ())), preferred_element_type=F32)


def pack_kernel(core_ref, qo_ref, do_ref, qp_ref, dp_ref, own_ref, oth_ref, qs, rs, ds):
    for q_ref, g_ref, out in ((qo_ref, do_ref, own_ref), (qp_ref, dp_ref, oth_ref)):
        qs[...] = q_ref[:, :, :D].astype(F32).reshape(TB * HC, D)
        rs[:, :R] = q_ref[:, :, D:].astype(F32).reshape(TB * HC, R)
        ds[...] = g_ref[...].astype(F32).reshape(TB * HC, D)
        for p in range(NP):
            ropes = []
            for k in range(2):
                h = 2 * p + k
                rows = pl.ds(h, TB, stride=HC)
                out[p, k] = qs[rows, :].astype(BF)
                out[p, 2 + k] = ds[rows, :].astype(BF)
                ropes.append(rs[rows, :][:, :R])
            out[p, 4] = jnp.concatenate(ropes, axis=1).astype(BF)


def pack_chunk(group, core, queries, d_out):
    j, units = group

    def own(i, c):
        return (0, c[0] * (64 // HC) + j + i, 0)

    def oth(i, c):
        return (0, (1 - c[0]) * (64 // HC) + j + i, 0)

    shape = jax.ShapeDtypeStruct((NP * units, 5, TB, D), BF)
    spec = pl.BlockSpec((NP, 5, TB, D), lambda i, c: (i, 0, 0, 0))
    return pl.pallas_call(
        pack_kernel,
        grid_spec=pltpu.PrefetchScalarGridSpec(
            num_scalar_prefetch=1, grid=(units,),
            in_specs=[pl.BlockSpec((TB, HC, D + R), own), pl.BlockSpec((TB, HC, D), own),
                      pl.BlockSpec((TB, HC, D + R), oth), pl.BlockSpec((TB, HC, D), oth)],
            out_specs=[spec, spec],
            scratch_shapes=[pltpu.VMEM((TB * HC, D), F32)] * 3),
        out_shape=[shape, shape],
        name="pack",
        cost_estimate=pl.CostEstimate(flops=10 ** 9, bytes_accessed=3 * 10 ** 6, transcendentals=0),
    )(core, queries, d_out, queries, d_out)


def prep_kernel(me_ref, *refs):
    ins, (c_ref, ct_ref, r_ref) = refs[:ND], refs[ND:]
    for d in range(ND):
        slot = pl.multiple_of(jnp.bitwise_xor(me_ref[0], d) * TB, TB)
        c = ins[d][:, :L]
        c_ref[pl.ds(slot, TB), :] = c
        ct_ref[:, pl.ds(slot, TB)] = c.astype(F32).T.astype(BF)
        r_ref[pl.ds(slot, TB), :] = ins[d][:, L:]


def prep(me, blocks):
    return pl.pallas_call(
        prep_kernel,
        grid_spec=pltpu.PrefetchScalarGridSpec(
            num_scalar_prefetch=1, grid=(1,),
            in_specs=[pl.BlockSpec((TB, L + D), lambda i, m: (0, 0))] * ND,
            out_specs=[pl.BlockSpec((S, L), lambda i, m: (0, 0)),
                       pl.BlockSpec((L, S), lambda i, m: (0, 0)),
                       pl.BlockSpec((S, D), lambda i, m: (0, 0))]),
        out_shape=[jax.ShapeDtypeStruct((S, L), BF), jax.ShapeDtypeStruct((L, S), BF),
                   jax.ShapeDtypeStruct((S, D), BF)],
        name="prep",
    )(me, *blocks)


def partner_dw(h0, scale, ct_ref, dkv_in, bigs):
    for w in range(2):
        view = bigs[w].reshape(L * HC, D)
        dw = dot(ct_ref[...], dkv_in[0, w], 1, 0)
        dw = dw * scale if w == 0 else dw
        for k in range(2):
            view[pl.ds(h0 + k, L, stride=HC), :] = dw[:, k * D:(k + 1) * D]


def main_kernel(aliased, lead, score_scale, me_ref, *refs):
    prev = lead > 0
    _, ct_ref, _, _, _, _, _ = refs[ND:ND + 7]
    n_in = ND + 7
    if prev:
        dkv_in, o_in, dq_in = refs[n_in:n_in + 3]
        n_in += 3
    outs = refs[n_in + (4 if aliased else 0):]
    (dwk_big, dwv_big, o_big, dq_big, dkv_out, o_par, dq_par, dc_out, dr_out, *scratch) = outs
    step = pl.program_id(0)
    if not prev:
        main_body(step, score_scale, me_ref, refs, outs)
        return

    @pl.when(step < lead)
    def _():
        partner_dw(2 * (step % NP), score_scale, ct_ref, dkv_in, (dwk_big, dwv_big))

    @pl.when((step < lead) & (step % NP == 0))
    def _():
        o_big[...] = o_in[...]
        dq_big[...] = dq_in[...]

    @pl.when(step >= lead)
    def _():
        main_body(step - lead, score_scale, me_ref, refs, outs)


def main_body(p_all, score_scale, me_ref, refs, outs):
    p = p_all % NP
    a_refs = refs[:ND]
    c_ref, ct_ref, r_ref, wk_ref, wv_ref, dc_in, dr_in = refs[ND:ND + 7]
    (dwk_big, dwv_big, o_big, dq_big, dkv_out, o_par, dq_par, dc_out, dr_out,
     wsc, wk, wv, kr, vs, qa, do, pt, dst, st, dp, dkr, osc, dqn, dqr, oacc, dqacc) = outs
    me = me_ref[0]
    core = jnp.bitwise_and(me, 1)
    chip = me // 2
    own_rows = pl.ds(pl.multiple_of(chip * QB, QB), QB)
    k2 = score_scale * math.log2(math.e)

    @pl.when(p == 0)
    def _():
        for src, dst_w in ((wk_ref, wk), (wv_ref, wv)):
            wsc[...] = src[...].astype(F32).reshape(L * HC, D)
            for h in range(HC):
                dst_w[h // 2, :, (h % 2) * D:(h % 2 + 1) * D] = wsc[pl.ds(h, L, stride=HC), :].astype(BF)

    @pl.when(p_all == 0)
    def _():
        r = r_ref[...]
        zero = jnp.zeros((S, R), BF)
        kr[0, :, D:] = jnp.concatenate([r[:, :R], zero], axis=1)
        kr[1, :, D:] = jnp.concatenate([zero, r[:, :R]], axis=1)
        for t in range(1, NQ):
            pt[t * QB:(t + 1) * QB, :t * QB] = jnp.zeros((QB, t * QB), BF)
            dst[t * QB:(t + 1) * QB, :t * QB] = jnp.zeros((QB, t * QB), BF)
        dc_out[...] = dc_in[...]
        dr_out[...] = dr_in[...]

    for d in range(ND):
        slot = pl.ds(pl.multiple_of(jnp.bitwise_xor(me, d) * TB, TB), TB)
        for k in range(2):
            qa[k, slot, :D] = a_refs[d][0, k]
            qa[k, slot, D:] = a_refs[d][0, 4]
            do[k, slot, :] = a_refs[d][0, 2 + k]

    keys = dot(c_ref[...], wk[p], 1, 0).astype(BF)
    vals = dot(c_ref[...], wv[p], 1, 0).astype(BF)
    for k in range(2):
        kr[k, :, :D] = keys[:, k * D:(k + 1) * D]
        vs[k] = vals[:, k * D:(k + 1) * D]

    low = lax.broadcasted_iota(jnp.int32, (8, QB), 0)
    col = lax.broadcasted_iota(jnp.int32, (8, QB), 1)

    @pl.loop(0, 2)
    def _(k):
        def scores(i):
            q_i = qa[k, i * QB:(i + 1) * QB, :]
            d_i = do[k, i * QB:(i + 1) * QB, :]
            base = QB * (i * (i + 1) // 2)
            rows = slice(0, (i + 1) * QB)
            out = slice(base, base + (i + 1) * QB)
            st[out, :] = dot(kr[k, rows, :], q_i, 1, 1)
            dp[out, :] = dot(vs[k, rows, :], d_i, 1, 1)

        def soften(i):
            n = (i + 1) * QB
            base = QB * (i * (i + 1) // 2)
            mxs = [None] * 4
            for r0 in range(0, n, 8):
                x = st[base + r0:base + r0 + 8, :]
                if r0 >= i * QB:
                    x = jnp.where(low + (r0 - i * QB) <= col, x, NEG)
                    st[base + r0:base + r0 + 8, :] = x
                a = r0 // 8 % 4
                mxs[a] = x if mxs[a] is None else jnp.maximum(mxs[a], x)
            mx = jnp.maximum(jnp.maximum(mxs[0], mxs[1]), jnp.maximum(mxs[2], mxs[3]))
            mx = jnp.max(mx, axis=0, keepdims=True)
            ls = jnp.zeros((8, QB), F32)
            ts = jnp.zeros((8, QB), F32)
            for r0 in range(base, base + n, ROWS):
                e = jnp.exp2((st[r0:r0 + ROWS, :] - mx) * k2)
                st[r0:r0 + ROWS, :] = e
                ls += jnp.sum(e.reshape(ROWS // 8, 8, QB), axis=0)
                ts += jnp.sum((e * dp[r0:r0 + ROWS, :]).reshape(ROWS // 8, 8, QB), axis=0)
            inv = 1.0 / jnp.sum(ls, axis=0, keepdims=True)
            delta = jnp.sum(ts, axis=0, keepdims=True) * inv
            for r0 in range(0, n, ROWS):
                prob = st[base + r0:base + r0 + ROWS, :] * inv
                pt[r0:r0 + ROWS, i * QB:n] = prob.astype(BF)
                dst[r0:r0 + ROWS, i * QB:n] = (prob * (dp[base + r0:base + r0 + ROWS, :] - delta)).astype(BF)

        def grads(t):
            rows = slice(t * QB, (t + 1) * QB)
            grad = dot(dst[rows, t * QB:], qa[k, t * QB:, :], 1, 0)
            dkr[rows, :] = grad[:, D:]
            lanes = pl.ds(pl.multiple_of(k * D, D), D)
            dkv_out[0, 0, rows, lanes] = grad[:, :D].astype(BF)
            dkv_out[0, 1, rows, lanes] = dot(pt[rows, t * QB:], do[k, t * QB:, :], 1, 0).astype(BF)

        scores(NQ - 1)
        for i in range(NQ - 1, -1, -1):
            if i:
                scores(i - 1)
            soften(i)
            grads(i)
        dr_out[k] += dkr[own_rows, :] * score_scale

        cols = pl.ds(pl.multiple_of(chip * QB, QB), QB)
        oacc[...] = dot(pt[:, cols], vs[k], 0, 0)
        dqacc[...] = dot(dst[:, cols], kr[k], 0, 0) * score_scale
        head = 2 * p + k
        for side in range(2):
            half = jnp.bitwise_xor(core, side)
            tok = pl.ds(pl.multiple_of(half * TB, TB), TB)
            rows = pl.ds(head, TB, stride=HC)
            osc[side, rows, :] = oacc[tok, :]
            dqn[side, rows, :] = dqacc[tok, :D]
            rope = dqacc[tok, D:]
            dqr[side, rows, :] = jnp.where(k == 0, rope, pltpu.roll(rope, R, 1))

    for g, w in enumerate((wk, wv)):
        d_lat = dot(dkv_out[0, g, own_rows, :], w[p], 1, 1)
        dc_out[...] += d_lat if g else d_lat * score_scale
    partner_dw(2 * p, score_scale, ct_ref, dkv_out, (dwk_big, dwv_big))

    @pl.when(p == NP - 1)
    def _():
        o_big[...] = osc[0].reshape(TB, HC, D).astype(BF)
        o_par[...] = osc[1].reshape(TB, HC, D).astype(BF)
        for side, dq in ((0, dq_big), (1, dq_par)):
            dq[:, :, :D] = dqn[side].reshape(TB, HC, D).astype(BF)
            dq[:, :, D:] = dqr[side].reshape(TB, HC, D)[:, :, :R].astype(BF)


def big_shapes():
    return [jax.ShapeDtypeStruct((L, 128, D), F32), jax.ShapeDtypeStruct((L, 128, D), F32),
            jax.ShapeDtypeStruct((TB, 128, D), BF), jax.ShapeDtypeStruct((TB, 128, D + R), BF)]


def main_chunk(group, score_scale, me, blocks, c_abs, c_t, r_abs, w_uk, w_uv, dc, dr, big, prev_group, prev):
    per = 64 // HC
    j, units = group
    j_prev, units_prev = prev_group if prev is not None else (0, 0)
    lead = NP * units_prev

    def main_unit(i):
        return jnp.maximum(i - lead, 0) // NP

    def prev_unit(i):
        return jnp.minimum(i, lead - 1) // NP

    def head_block(i, m):
        return (0, (m[0] % 2) * per + j + main_unit(i), 0)

    def out_block(i, m):
        own = (m[0] % 2) * per + j + main_unit(i)
        if not lead:
            return (0, own, 0)
        return (0, jnp.where(i < lead, (1 - m[0] % 2) * per + j_prev + prev_unit(i), own), 0)

    def par_block(i, m):
        return (0, main_unit(i), 0)

    def in_block(i, m):
        return (0, prev_unit(i), 0)

    def main_step(i, m):
        return (jnp.maximum(i - lead, 0), 0, 0, 0)

    def prev_step(i, m):
        return (jnp.minimum(i, lead - 1), 0, 0, 0)

    def full2(i, m):
        return (0, 0)

    def full3(i, m):
        return (0, 0, 0)

    once = pl.Buffered(1)
    in_specs = ([pl.BlockSpec((1, 5, TB, D), main_step)] * ND
                + [pl.BlockSpec((S, L), full2, pipeline_mode=once),
                   pl.BlockSpec((L, S), full2, pipeline_mode=once),
                   pl.BlockSpec((S, D), full2, pipeline_mode=once),
                   pl.BlockSpec((L, HC, D), head_block),
                   pl.BlockSpec((L, HC, D), head_block),
                   pl.BlockSpec((QB, L), full2, pipeline_mode=once),
                   pl.BlockSpec((2, QB, D), full3, pipeline_mode=once)])
    args = list(blocks) + [c_abs, c_t, r_abs, w_uk, w_uv, dc, dr]
    if prev is not None:
        in_specs += [pl.BlockSpec((1, 2, S, 2 * D), prev_step),
                     pl.BlockSpec((TB, HC, D), in_block), pl.BlockSpec((TB, HC, D + R), in_block)]
        args += list(prev)
    aliases = {}
    if big is not None:
        in_specs += [pl.BlockSpec(memory_space=pl.ANY)] * 4
        aliases = {1 + len(args) + b: b for b in range(4)}
        args += list(big)
    tri = QB * NQ * (NQ + 1) // 2
    outs = pl.pallas_call(
        functools.partial(main_kernel, big is not None, lead, score_scale),
        grid_spec=pltpu.PrefetchScalarGridSpec(
            num_scalar_prefetch=1, grid=(NP * units + lead,),
            in_specs=in_specs,
            out_specs=[pl.BlockSpec((L, HC, D), out_block),
                       pl.BlockSpec((L, HC, D), out_block),
                       pl.BlockSpec((TB, HC, D), out_block),
                       pl.BlockSpec((TB, HC, D + R), out_block),
                       pl.BlockSpec((1, 2, S, 2 * D), main_step),
                       pl.BlockSpec((TB, HC, D), par_block), pl.BlockSpec((TB, HC, D + R), par_block),
                       pl.BlockSpec((QB, L), full2, pipeline_mode=once),
                       pl.BlockSpec((2, QB, D), full3, pipeline_mode=once)],
            scratch_shapes=[
                pltpu.VMEM((L * HC, D), F32),
                pltpu.VMEM((NP, L, 2 * D), BF), pltpu.VMEM((NP, L, 2 * D), BF),
                pltpu.VMEM((2, S, 2 * D), BF), pltpu.VMEM((2, S, D), BF),
                pltpu.VMEM((2, S, 2 * D), BF), pltpu.VMEM((2, S, D), BF),
                pltpu.VMEM((S, S), BF), pltpu.VMEM((S, S), BF),
                pltpu.VMEM((tri, QB), F32), pltpu.VMEM((tri, QB), F32),
                pltpu.VMEM((S, D), F32),
                pltpu.VMEM((2, TB * HC, D), F32), pltpu.VMEM((2, TB * HC, D), F32),
                pltpu.VMEM((2, TB * HC, D), F32),
                pltpu.VMEM((QB, D), F32), pltpu.VMEM((QB, 2 * D), F32)]),
        out_shape=big_shapes() + [
            jax.ShapeDtypeStruct((NP * units, 2, S, 2 * D), BF),
            jax.ShapeDtypeStruct((TB, HC * units, D), BF),
            jax.ShapeDtypeStruct((TB, HC * units, D + R), BF),
            jax.ShapeDtypeStruct((QB, L), F32), jax.ShapeDtypeStruct((2, QB, D), F32)],
        input_output_aliases=aliases,
        compiler_params=pltpu.CompilerParams(vmem_limit_bytes=60 * 2 ** 20),
        name="mla_chunk",
        cost_estimate=pl.CostEstimate(flops=units * 25 * 10 ** 9, bytes_accessed=20 * 10 ** 6, transcendentals=0),
    )(me, *args)
    return outs[:4], outs[4:7], outs[7], outs[8]


def last_kernel(score_scale, core_ref, ct_ref, dkv_in, o_in, dq_in, *refs):
    dwk_big, dwv_big, o_big, dq_big = refs[4:]
    step = pl.program_id(0)
    partner_dw(2 * (step % NP), score_scale, ct_ref, dkv_in, (dwk_big, dwv_big))

    @pl.when(step % NP == 0)
    def _():
        o_big[...] = o_in[...]
        dq_big[...] = dq_in[...]


def last_chunk(group, score_scale, core, c_t, prev, big):
    j, units = group

    def at(i, c):
        return (0, (1 - c[0]) * (64 // HC) + j + i // NP, 0)

    def full3(i, c):
        return (0, i // NP, 0)

    return pl.pallas_call(
        functools.partial(last_kernel, score_scale),
        grid_spec=pltpu.PrefetchScalarGridSpec(
            num_scalar_prefetch=1, grid=(NP * units,),
            in_specs=[pl.BlockSpec((L, S), lambda i, c: (0, 0), pipeline_mode=pl.Buffered(1)),
                      pl.BlockSpec((1, 2, S, 2 * D), lambda i, c: (i, 0, 0, 0)),
                      pl.BlockSpec((TB, HC, D), full3), pl.BlockSpec((TB, HC, D + R), full3)]
                     + [pl.BlockSpec(memory_space=pl.ANY)] * 4,
            out_specs=[pl.BlockSpec((L, HC, D), at), pl.BlockSpec((L, HC, D), at),
                       pl.BlockSpec((TB, HC, D), at), pl.BlockSpec((TB, HC, D + R), at)]),
        out_shape=big_shapes(),
        input_output_aliases={5 + b: b for b in range(4)},
        compiler_params=pltpu.CompilerParams(vmem_limit_bytes=40 * 2 ** 20),
        name="last",
        cost_estimate=pl.CostEstimate(flops=2 * 10 ** 9, bytes_accessed=10 ** 7, transcendentals=0),
    )(core, c_t, *prev, *big)


def solution(mesh):
    def hop(x, k):
        perm = [(i, i ^ k) for i in range(ND)]
        return lax.ppermute(x, "cp", perm)

    def step(queries, latent, key_rope, w_uk, w_uv, d_out):
        score_scale = 1.0 / math.sqrt(queries.shape[-1])
        dev = lax.axis_index("cp").astype(jnp.int32)
        me = dev[None]
        core = me % 2
        n_chunks = len(GROUPS)
        groups = [(sum(GROUPS[:g]), GROUPS[g]) for g in range(n_chunks)]

        lat = jnp.concatenate([latent, key_rope, jnp.zeros((TB, D - R), BF)], axis=1)
        lats = [lat] + [hop(lat, k) for k in range(1, ND)]
        queries, lat1 = lax.optimization_barrier((queries, lats[1]))
        lats[1] = lat1
        c_abs, c_t, r_abs = prep(me, lats)

        packs = []
        for group in groups:
            packs.append(pack_chunk(group, core, queries, d_out))
        recv = []
        for own, oth in packs:
            a1, a2, a5, a3, a4 = [hop(x, k)
                                  for x, k in ((oth, 1), (own, 2), (oth, 5), (oth, 3), (own, 4))]
            a6, a7 = hop(a2, 4), hop(a5, 2)
            recv.append([own, a1, a2, a3, a4, a5, a6, a7])

        dc = jnp.zeros((QB, L), F32)
        dr = jnp.zeros((2, QB, D), F32)
        big = None
        sent = []
        for j in range(n_chunks):
            big, send, dc, dr = main_chunk(groups[j], score_scale, me, recv[j],
                                           c_abs, c_t, r_abs, w_uk, w_uv, dc, dr, big,
                                           groups[j - 2] if j >= 2 else None,
                                           sent[j - 2] if j >= 2 else None)
            sent.append([hop(x, 1) for x in send])
        dc = dc.reshape(2, TB, L)
        dr = dr[0, :, :R] + dr[1, :, R:]
        dr = dr.reshape(2, TB, R)
        c_idx = core[0]

        def swap_sum(x):
            mine = lax.dynamic_index_in_dim(x, c_idx, 0, keepdims=False)
            theirs = lax.dynamic_index_in_dim(x, 1 - c_idx, 0, keepdims=False)
            return (mine + hop(theirs, 1)).astype(BF)

        d_latent = swap_sum(dc)
        d_key_rope = swap_sum(dr)
        for j in (n_chunks - 2, n_chunks - 1):
            big = last_chunk(groups[j], score_scale, core, c_t, sent[j], big)
        d_w_uk, d_w_uv, attn_out, d_query = big
        return attn_out, d_query, d_latent, d_key_rope, d_w_uk, d_w_uv

    seq = P("cp")
    return jax.shard_map(step, mesh=mesh,
                         in_specs=(seq, seq, seq, P(), P(), seq),
                         out_specs=(seq, seq, seq, seq, P(), P()),
                         check_vma=False)
```

```python
import functools
import math
import jax
import jax.numpy as jnp
from jax import lax
from jax.experimental import pallas as pl
from jax.experimental.pallas import tpu as pltpu
from jax.sharding import PartitionSpec as P


TB = 128
ND = 8
S = TB * ND
QB = 256
NQ = S // QB
HC = 8
NP = HC // 2
L = 512
D = 128
R = 64
ROWS = 32
NEG = -1e30
BF = jnp.bfloat16
GROUPS = (1, 1, 1, 1, 1, 2, 1)
F32 = jnp.float32


def dot(a, b, ca, cb):
    return lax.dot_general(a, b, (((ca,), (cb,)), ((), ())), preferred_element_type=F32)


def pack_kernel(core_ref, qo_ref, do_ref, qp_ref, dp_ref, own_ref, oth_ref, qs, rs, ds):
    for q_ref, g_ref, out in ((qo_ref, do_ref, own_ref), (qp_ref, dp_ref, oth_ref)):
        qs[...] = q_ref[:, :, :D].astype(F32).reshape(TB * HC, D)
        rs[:, :R] = q_ref[:, :, D:].astype(F32).reshape(TB * HC, R)
        ds[...] = g_ref[...].astype(F32).reshape(TB * HC, D)
        for p in range(NP):
            ropes = []
            for k in range(2):
                h = 2 * p + k
                rows = pl.ds(h, TB, stride=HC)
                out[p, k] = qs[rows, :].astype(BF)
                out[p, 2 + k] = ds[rows, :].astype(BF)
                ropes.append(rs[rows, :][:, :R])
            out[p, 4] = jnp.concatenate(ropes, axis=1).astype(BF)


def pack_chunk(group, core, queries, d_out):
    j, units = group

    def own(i, c):
        return (0, c[0] * (64 // HC) + j + i, 0)

    def oth(i, c):
        return (0, (1 - c[0]) * (64 // HC) + j + i, 0)

    shape = jax.ShapeDtypeStruct((NP * units, 5, TB, D), BF)
    spec = pl.BlockSpec((NP, 5, TB, D), lambda i, c: (i, 0, 0, 0))
    return pl.pallas_call(
        pack_kernel,
        grid_spec=pltpu.PrefetchScalarGridSpec(
            num_scalar_prefetch=1, grid=(units,),
            in_specs=[pl.BlockSpec((TB, HC, D + R), own), pl.BlockSpec((TB, HC, D), own),
                      pl.BlockSpec((TB, HC, D + R), oth), pl.BlockSpec((TB, HC, D), oth)],
            out_specs=[spec, spec],
            scratch_shapes=[pltpu.VMEM((TB * HC, D), F32)] * 3),
        out_shape=[shape, shape],
        name="pack",
        cost_estimate=pl.CostEstimate(flops=10 ** 9, bytes_accessed=3 * 10 ** 6, transcendentals=0),
    )(core, queries, d_out, queries, d_out)


def prep_kernel(me_ref, *refs):
    ins, (c_ref, ct_ref, r_ref) = refs[:ND], refs[ND:]
    for d in range(ND):
        slot = pl.multiple_of(jnp.bitwise_xor(me_ref[0], d) * TB, TB)
        c = ins[d][:, :L]
        c_ref[pl.ds(slot, TB), :] = c
        ct_ref[:, pl.ds(slot, TB)] = c.astype(F32).T.astype(BF)
        r_ref[pl.ds(slot, TB), :] = ins[d][:, L:]


def prep(me, blocks):
    return pl.pallas_call(
        prep_kernel,
        grid_spec=pltpu.PrefetchScalarGridSpec(
            num_scalar_prefetch=1, grid=(1,),
            in_specs=[pl.BlockSpec((TB, L + D), lambda i, m: (0, 0))] * ND,
            out_specs=[pl.BlockSpec((S, L), lambda i, m: (0, 0)),
                       pl.BlockSpec((L, S), lambda i, m: (0, 0)),
                       pl.BlockSpec((S, D), lambda i, m: (0, 0))]),
        out_shape=[jax.ShapeDtypeStruct((S, L), BF), jax.ShapeDtypeStruct((L, S), BF),
                   jax.ShapeDtypeStruct((S, D), BF)],
        name="prep",
    )(me, *blocks)


def partner_dw(h0, scale, ct_ref, dkv_in, bigs):
    for w in range(2):
        view = bigs[w].reshape(L * HC, D)
        dw = dot(ct_ref[...], dkv_in[0, w], 1, 0)
        dw = dw * scale if w == 0 else dw
        for k in range(2):
            view[pl.ds(h0 + k, L, stride=HC), :] = dw[:, k * D:(k + 1) * D]


def main_kernel(aliased, lead, score_scale, me_ref, *refs):
    prev = lead > 0
    _, ct_ref, _, _, _, _, _ = refs[ND:ND + 7]
    n_in = ND + 7
    if prev:
        dkv_in, o_in, dq_in = refs[n_in:n_in + 3]
        n_in += 3
    outs = refs[n_in + (4 if aliased else 0):]
    (dwk_big, dwv_big, o_big, dq_big, dkv_out, o_par, dq_par, dc_out, dr_out, *scratch) = outs
    step = pl.program_id(0)
    if not prev:
        main_body(step, score_scale, me_ref, refs, outs)
        return

    @pl.when(step < lead)
    def _():
        partner_dw(2 * (step % NP), score_scale, ct_ref, dkv_in, (dwk_big, dwv_big))

    @pl.when((step < lead) & (step % NP == 0))
    def _():
        o_big[...] = o_in[...]
        dq_big[...] = dq_in[...]

    @pl.when(step >= lead)
    def _():
        main_body(step - lead, score_scale, me_ref, refs, outs)


def main_body(p_all, score_scale, me_ref, refs, outs):
    p = p_all % NP
    a_refs = refs[:ND]
    c_ref, ct_ref, r_ref, wk_ref, wv_ref, dc_in, dr_in = refs[ND:ND + 7]
    (dwk_big, dwv_big, o_big, dq_big, dkv_out, o_par, dq_par, dc_out, dr_out,
     wsc, wk, wv, kr, vs, qa, do, pt, dst, st, dp, dkr, osc, dqn, dqr, oacc, dqacc) = outs
    me = me_ref[0]
    core = jnp.bitwise_and(me, 1)
    chip = me // 2
    own_rows = pl.ds(pl.multiple_of(chip * QB, QB), QB)
    k2 = score_scale * math.log2(math.e)

    @pl.when(p == 0)
    def _():
        for src, dst_w in ((wk_ref, wk), (wv_ref, wv)):
            wsc[...] = src[...].astype(F32).reshape(L * HC, D)
            for h in range(HC):
                dst_w[h // 2, :, (h % 2) * D:(h % 2 + 1) * D] = wsc[pl.ds(h, L, stride=HC), :].astype(BF)

    @pl.when(p_all == 0)
    def _():
        r = r_ref[...]
        zero = jnp.zeros((S, R), BF)
        kr[0, :, D:] = jnp.concatenate([r[:, :R], zero], axis=1)
        kr[1, :, D:] = jnp.concatenate([zero, r[:, :R]], axis=1)
        for t in range(1, NQ):
            pt[t * QB:(t + 1) * QB, :t * QB] = jnp.zeros((QB, t * QB), BF)
            dst[t * QB:(t + 1) * QB, :t * QB] = jnp.zeros((QB, t * QB), BF)
        dc_out[...] = dc_in[...]
        dr_out[...] = dr_in[...]

    for d in range(ND):
        slot = pl.ds(pl.multiple_of(jnp.bitwise_xor(me, d) * TB, TB), TB)
        for k in range(2):
            qa[k, slot, :D] = a_refs[d][0, k]
            qa[k, slot, D:] = a_refs[d][0, 4]
            do[k, slot, :] = a_refs[d][0, 2 + k]

    keys = dot(c_ref[...], wk[p], 1, 0).astype(BF)
    vals = dot(c_ref[...], wv[p], 1, 0).astype(BF)
    for k in range(2):
        kr[k, :, :D] = keys[:, k * D:(k + 1) * D]
        vs[k] = vals[:, k * D:(k + 1) * D]

    upper = lax.broadcasted_iota(jnp.int32, (QB, QB), 0) <= lax.broadcasted_iota(jnp.int32, (QB, QB), 1)

    @pl.loop(0, 2)
    def _(k):
        def scores(i):
            q_i = qa[k, i * QB:(i + 1) * QB, :]
            d_i = do[k, i * QB:(i + 1) * QB, :]
            base = QB * (i * (i + 1) // 2)
            for t in range(i + 1):
                rows = slice(t * QB, (t + 1) * QB)
                out = slice(base + t * QB, base + (t + 1) * QB)
                sc = dot(kr[k, rows, :], q_i, 1, 1)
                st[out, :] = jnp.where(upper, sc, NEG) if t == i else sc
                dp[out, :] = dot(vs[k, rows, :], d_i, 1, 1)

        def soften(i):
            n = (i + 1) * QB
            base = QB * (i * (i + 1) // 2)
            mxs = [st[base + 8 * a:base + 8 * a + 8, :] for a in range(4)]
            for r0 in range(32, n, 32):
                for a in range(4):
                    mxs[a] = jnp.maximum(mxs[a], st[base + r0 + 8 * a:base + r0 + 8 * a + 8, :])
            mx = jnp.maximum(jnp.maximum(mxs[0], mxs[1]), jnp.maximum(mxs[2], mxs[3]))
            mx = jnp.max(mx, axis=0, keepdims=True)
            ls = jnp.zeros((8, QB), F32)
            ts = jnp.zeros((8, QB), F32)
            for r0 in range(base, base + n, ROWS):
                e = jnp.exp2((st[r0:r0 + ROWS, :] - mx) * k2)
                st[r0:r0 + ROWS, :] = e
                ls += jnp.sum(e.reshape(ROWS // 8, 8, QB), axis=0)
                ts += jnp.sum((e * dp[r0:r0 + ROWS, :]).reshape(ROWS // 8, 8, QB), axis=0)
            inv = 1.0 / jnp.sum(ls, axis=0, keepdims=True)
            delta = jnp.sum(ts, axis=0, keepdims=True) * inv
            for r0 in range(0, n, ROWS):
                prob = st[base + r0:base + r0 + ROWS, :] * inv
                pt[r0:r0 + ROWS, i * QB:n] = prob.astype(BF)
                dst[r0:r0 + ROWS, i * QB:n] = (prob * (dp[base + r0:base + r0 + ROWS, :] - delta)).astype(BF)

        def grads(t):
            rows = slice(t * QB, (t + 1) * QB)
            grad = dot(dst[rows, t * QB:], qa[k, t * QB:, :], 1, 0)
            dkr[rows, :] = grad[:, D:]
            lanes = pl.ds(pl.multiple_of(k * D, D), D)
            dkv_out[0, 0, rows, lanes] = grad[:, :D].astype(BF)
            dkv_out[0, 1, rows, lanes] = dot(pt[rows, t * QB:], do[k, t * QB:, :], 1, 0).astype(BF)

        scores(NQ - 1)
        for i in range(NQ - 1, -1, -1):
            if i:
                scores(i - 1)
            soften(i)
            grads(i)
        dr_out[k] += dkr[own_rows, :] * score_scale

        cols = pl.ds(pl.multiple_of(chip * QB, QB), QB)
        oacc[...] = dot(pt[:, cols], vs[k], 0, 0)
        dqacc[...] = dot(dst[:, cols], kr[k], 0, 0) * score_scale
        head = 2 * p + k
        for side in range(2):
            half = jnp.bitwise_xor(core, side)
            tok = pl.ds(pl.multiple_of(half * TB, TB), TB)
            rows = pl.ds(head, TB, stride=HC)
            osc[side, rows, :] = oacc[tok, :]
            dqn[side, rows, :] = dqacc[tok, :D]
            rope = dqacc[tok, D:]
            dqr[side, rows, :] = jnp.where(k == 0, rope, pltpu.roll(rope, R, 1))

    for g, w in enumerate((wk, wv)):
        d_lat = dot(dkv_out[0, g, own_rows, :], w[p], 1, 1)
        dc_out[...] += d_lat if g else d_lat * score_scale
    partner_dw(2 * p, score_scale, ct_ref, dkv_out, (dwk_big, dwv_big))

    @pl.when(p == NP - 1)
    def _():
        o_big[...] = osc[0].reshape(TB, HC, D).astype(BF)
        o_par[...] = osc[1].reshape(TB, HC, D).astype(BF)
        for side, dq in ((0, dq_big), (1, dq_par)):
            dq[:, :, :D] = dqn[side].reshape(TB, HC, D).astype(BF)
            dq[:, :, D:] = dqr[side].reshape(TB, HC, D)[:, :, :R].astype(BF)


def big_shapes():
    return [jax.ShapeDtypeStruct((L, 128, D), F32), jax.ShapeDtypeStruct((L, 128, D), F32),
            jax.ShapeDtypeStruct((TB, 128, D), BF), jax.ShapeDtypeStruct((TB, 128, D + R), BF)]


def main_chunk(group, score_scale, me, blocks, c_abs, c_t, r_abs, w_uk, w_uv, dc, dr, big, prev_group, prev):
    per = 64 // HC
    j, units = group
    j_prev, units_prev = prev_group if prev is not None else (0, 0)
    lead = NP * units_prev

    def main_unit(i):
        return jnp.maximum(i - lead, 0) // NP

    def prev_unit(i):
        return jnp.minimum(i, lead - 1) // NP

    def head_block(i, m):
        return (0, (m[0] % 2) * per + j + main_unit(i), 0)

    def out_block(i, m):
        own = (m[0] % 2) * per + j + main_unit(i)
        if not lead:
            return (0, own, 0)
        return (0, jnp.where(i < lead, (1 - m[0] % 2) * per + j_prev + prev_unit(i), own), 0)

    def par_block(i, m):
        return (0, main_unit(i), 0)

    def in_block(i, m):
        return (0, prev_unit(i), 0)

    def main_step(i, m):
        return (jnp.maximum(i - lead, 0), 0, 0, 0)

    def prev_step(i, m):
        return (jnp.minimum(i, lead - 1), 0, 0, 0)

    def full2(i, m):
        return (0, 0)

    def full3(i, m):
        return (0, 0, 0)

    once = pl.Buffered(1)
    in_specs = ([pl.BlockSpec((1, 5, TB, D), main_step)] * ND
                + [pl.BlockSpec((S, L), full2, pipeline_mode=once),
                   pl.BlockSpec((L, S), full2, pipeline_mode=once),
                   pl.BlockSpec((S, D), full2, pipeline_mode=once),
                   pl.BlockSpec((L, HC, D), head_block),
                   pl.BlockSpec((L, HC, D), head_block),
                   pl.BlockSpec((QB, L), full2, pipeline_mode=once),
                   pl.BlockSpec((2, QB, D), full3, pipeline_mode=once)])
    args = list(blocks) + [c_abs, c_t, r_abs, w_uk, w_uv, dc, dr]
    if prev is not None:
        in_specs += [pl.BlockSpec((1, 2, S, 2 * D), prev_step),
                     pl.BlockSpec((TB, HC, D), in_block), pl.BlockSpec((TB, HC, D + R), in_block)]
        args += list(prev)
    aliases = {}
    if big is not None:
        in_specs += [pl.BlockSpec(memory_space=pl.ANY)] * 4
        aliases = {1 + len(args) + b: b for b in range(4)}
        args += list(big)
    tri = QB * NQ * (NQ + 1) // 2
    outs = pl.pallas_call(
        functools.partial(main_kernel, big is not None, lead, score_scale),
        grid_spec=pltpu.PrefetchScalarGridSpec(
            num_scalar_prefetch=1, grid=(NP * units + lead,),
            in_specs=in_specs,
            out_specs=[pl.BlockSpec((L, HC, D), out_block),
                       pl.BlockSpec((L, HC, D), out_block),
                       pl.BlockSpec((TB, HC, D), out_block),
                       pl.BlockSpec((TB, HC, D + R), out_block),
                       pl.BlockSpec((1, 2, S, 2 * D), main_step),
                       pl.BlockSpec((TB, HC, D), par_block), pl.BlockSpec((TB, HC, D + R), par_block),
                       pl.BlockSpec((QB, L), full2, pipeline_mode=once),
                       pl.BlockSpec((2, QB, D), full3, pipeline_mode=once)],
            scratch_shapes=[
                pltpu.VMEM((L * HC, D), F32),
                pltpu.VMEM((NP, L, 2 * D), BF), pltpu.VMEM((NP, L, 2 * D), BF),
                pltpu.VMEM((2, S, 2 * D), BF), pltpu.VMEM((2, S, D), BF),
                pltpu.VMEM((2, S, 2 * D), BF), pltpu.VMEM((2, S, D), BF),
                pltpu.VMEM((S, S), BF), pltpu.VMEM((S, S), BF),
                pltpu.VMEM((tri, QB), F32), pltpu.VMEM((tri, QB), F32),
                pltpu.VMEM((S, D), F32),
                pltpu.VMEM((2, TB * HC, D), F32), pltpu.VMEM((2, TB * HC, D), F32),
                pltpu.VMEM((2, TB * HC, D), F32),
                pltpu.VMEM((QB, D), F32), pltpu.VMEM((QB, 2 * D), F32)]),
        out_shape=big_shapes() + [
            jax.ShapeDtypeStruct((NP * units, 2, S, 2 * D), BF),
            jax.ShapeDtypeStruct((TB, HC * units, D), BF),
            jax.ShapeDtypeStruct((TB, HC * units, D + R), BF),
            jax.ShapeDtypeStruct((QB, L), F32), jax.ShapeDtypeStruct((2, QB, D), F32)],
        input_output_aliases=aliases,
        compiler_params=pltpu.CompilerParams(vmem_limit_bytes=60 * 2 ** 20),
        name="mla_chunk",
        cost_estimate=pl.CostEstimate(flops=units * 25 * 10 ** 9, bytes_accessed=20 * 10 ** 6, transcendentals=0),
    )(me, *args)
    return outs[:4], outs[4:7], outs[7], outs[8]


def last_kernel(score_scale, core_ref, ct_ref, dkv_in, o_in, dq_in, *refs):
    dwk_big, dwv_big, o_big, dq_big = refs[4:]
    step = pl.program_id(0)
    partner_dw(2 * (step % NP), score_scale, ct_ref, dkv_in, (dwk_big, dwv_big))

    @pl.when(step % NP == 0)
    def _():
        o_big[...] = o_in[...]
        dq_big[...] = dq_in[...]


def last_chunk(group, score_scale, core, c_t, prev, big):
    j, units = group

    def at(i, c):
        return (0, (1 - c[0]) * (64 // HC) + j + i // NP, 0)

    def full3(i, c):
        return (0, i // NP, 0)

    return pl.pallas_call(
        functools.partial(last_kernel, score_scale),
        grid_spec=pltpu.PrefetchScalarGridSpec(
            num_scalar_prefetch=1, grid=(NP * units,),
            in_specs=[pl.BlockSpec((L, S), lambda i, c: (0, 0), pipeline_mode=pl.Buffered(1)),
                      pl.BlockSpec((1, 2, S, 2 * D), lambda i, c: (i, 0, 0, 0)),
                      pl.BlockSpec((TB, HC, D), full3), pl.BlockSpec((TB, HC, D + R), full3)]
                     + [pl.BlockSpec(memory_space=pl.ANY)] * 4,
            out_specs=[pl.BlockSpec((L, HC, D), at), pl.BlockSpec((L, HC, D), at),
                       pl.BlockSpec((TB, HC, D), at), pl.BlockSpec((TB, HC, D + R), at)]),
        out_shape=big_shapes(),
        input_output_aliases={5 + b: b for b in range(4)},
        compiler_params=pltpu.CompilerParams(vmem_limit_bytes=60 * 2 ** 20),
        name="last",
        cost_estimate=pl.CostEstimate(flops=2 * 10 ** 9, bytes_accessed=10 ** 7, transcendentals=0),
    )(core, c_t, *prev, *big)


def solution(mesh):
    def hop(x, k):
        perm = [(i, i ^ k) for i in range(ND)]
        return lax.ppermute(x, "cp", perm)

    def step(queries, latent, key_rope, w_uk, w_uv, d_out):
        score_scale = 1.0 / math.sqrt(queries.shape[-1])
        dev = lax.axis_index("cp").astype(jnp.int32)
        me = dev[None]
        core = me % 2
        n_chunks = len(GROUPS)
        groups = [(sum(GROUPS[:g]), GROUPS[g]) for g in range(n_chunks)]

        lat = jnp.concatenate([latent, key_rope, jnp.zeros((TB, D - R), BF)], axis=1)
        lats = [lat] + [hop(lat, k) for k in range(1, ND)]
        queries, lat1 = lax.optimization_barrier((queries, lats[1]))
        lats[1] = lat1
        c_abs, c_t, r_abs = prep(me, lats)

        packs = []
        for group in groups:
            packs.append(pack_chunk(group, core, queries, d_out))
        recv = []
        for own, oth in packs:
            a1, a2, a5, a3, a4 = [hop(x, k)
                                  for x, k in ((oth, 1), (own, 2), (oth, 5), (oth, 3), (own, 4))]
            a6, a7 = hop(a2, 4), hop(a5, 2)
            recv.append([own, a1, a2, a3, a4, a5, a6, a7])

        dc = jnp.zeros((QB, L), F32)
        dr = jnp.zeros((2, QB, D), F32)
        big = None
        sent = []
        for j in range(n_chunks):
            big, send, dc, dr = main_chunk(groups[j], score_scale, me, recv[j],
                                           c_abs, c_t, r_abs, w_uk, w_uv, dc, dr, big,
                                           groups[j - 2] if j >= 2 else None,
                                           sent[j - 2] if j >= 2 else None)
            sent.append([hop(x, 1) for x in send])
        dc = dc.reshape(2, TB, L)
        dr = dr[0, :, :R] + dr[1, :, R:]
        dr = dr.reshape(2, TB, R)
        c_idx = core[0]

        def swap_sum(x):
            mine = lax.dynamic_index_in_dim(x, c_idx, 0, keepdims=False)
            theirs = lax.dynamic_index_in_dim(x, 1 - c_idx, 0, keepdims=False)
            return (mine + hop(theirs, 1)).astype(BF)

        d_latent = swap_sum(dc)
        d_key_rope = swap_sum(dr)
        for j in (n_chunks - 2, n_chunks - 1):
            big = last_chunk(groups[j], score_scale, core, c_t, sent[j], big)
        d_w_uk, d_w_uv, attn_out, d_query = big
        return attn_out, d_query, d_latent, d_key_rope, d_w_uk, d_w_uv

    seq = P("cp")
    return jax.shard_map(step, mesh=mesh,
                         in_specs=(seq, seq, seq, P(), P(), seq),
                         out_specs=(seq, seq, seq, seq, P(), P()),
                         check_vma=False)
```
